32 devices in a mesh: data: 2 (over x), outer: 4 (over z), expert: 4 (over y, core).
Axes of the slice: x: 2, y: 2, z: 4, core: 2. Of those that a mesh axis runs over, the one named last changes fastest.
Arguments:
- x: bfloat16 [16384, 2048], P(('data', 'outer', 'expert')), parts along dimension 0
- wr: bfloat16 [2048, 64], replicated
- idx: int32 [16384, 8], P(('data', 'outer', 'expert')), parts along dimension 0
- w1: bfloat16 [64, 2048, 1024], P(('outer', 'expert'))
- w3: bfloat16 [64, 2048, 1024], P(('outer', 'expert'))
- w2: bfloat16 [64, 1024, 2048], P(('outer', 'expert'))
Outputs:
- output: bfloat16 [16384, 2048], P(('data', 'outer', 'expert')), parts along dimension 0
There are 2 independent parts. The reference program is written for one: setup_inputs(seed, part) draws one part's arguments, and reference() takes and returns one part's arrays. A program takes and returns all parts, laid end to end along the dimension named above; an argument that names none is the same for every part.
All inputs are finite; a program needn't handle non-finite values.
Results may differ from the reference program's by a relative error of at most 0.00814968.
Values are sent between devices in bfloat16 or wider.
A program may use at most 1 GiB of HBM per device.

```python
import jax
import jax.numpy as jnp
from jax import lax

OUTER = 4
EXPERT = 4
T = 512
D = 2048
FF = 1024
E = 64
TOP = 8

N_DEV = OUTER * EXPERT
CAP = 2 * T * TOP // E


def _w(key, shape, scale):
    ks = jax.random.split(key, shape[0])
    return lax.map(lambda kk: (scale * jax.random.normal(kk, shape[1:], jnp.float32)).astype(jnp.bfloat16), ks)


def setup_inputs(seed: int = 0, part: int = 0) -> dict:
    key = jax.random.key(seed)
    kr, k1, k3, k2 = jax.random.split(key, 4)
    kp = jax.random.fold_in(key, part)
    kx, _, _ = jax.random.split(kp, 3)
    kb1, kb2, kb3 = jax.random.split(jax.random.fold_in(kp, 7), 3)
    x = jax.random.normal(kx, (N_DEV * T, D), jnp.float32).astype(jnp.bfloat16)
    wr = (1.5 * D ** -0.5 * jax.random.normal(kr, (D, E), jnp.float32)).astype(jnp.bfloat16)
    w1 = _w(k1, (E, D, FF), D ** -0.5)
    w3 = _w(k3, (E, D, FF), D ** -0.5)
    w2 = _w(k2, (E, FF, D), FF ** -0.5)
    nc = N_DEV * T // E
    rot = jax.random.randint(kb1, (N_DEV,), 0, E, jnp.int32)
    base = jnp.arange(E, dtype=jnp.int32) // 2
    p = jax.vmap(lambda kk: jax.random.permutation(kk, base))(jax.random.split(kb2, nc))
    p = p + jnp.repeat(rot, T // E)[:, None]
    w = min(2 * TOP, E)
    off = jax.vmap(lambda kk: jax.random.permutation(kk, w)[:TOP])(jax.random.split(kb3, nc))
    idx = ((p[:, :, None] + off[:, None, :]) % E).reshape(N_DEV * T, TOP).astype(jnp.int32)
    return {'x': x, 'wr': wr, 'idx': idx, 'w1': w1, 'w3': w3, 'w2': w2}


def _ranks(e, num):
    order = jnp.argsort(e, stable=True)
    se = e[order]
    first = jnp.searchsorted(se, jnp.arange(num, dtype=jnp.int32), side='left').astype(jnp.int32)
    r = jnp.arange(e.shape[0], dtype=jnp.int32) - first[se]
    return jnp.zeros_like(e).at[order].set(r)


def reference(x, wr, idx, w1, w3, w2):
    logits = jnp.dot(x, wr, preferred_element_type=jnp.float32)
    g = jax.nn.softmax(jnp.take_along_axis(logits, idx, axis=1), axis=-1)
    eb = idx.reshape(N_DEV, T * TOP)
    r = jax.vmap(lambda v: _ranks(v, E))(eb).reshape(-1)
    e = eb.reshape(-1)
    src = jnp.arange(N_DEV * T * TOP, dtype=jnp.int32) // (T * TOP)
    tok = jnp.arange(N_DEV * T * TOP, dtype=jnp.int32) // TOP
    pos = jnp.where(r < CAP, e * (N_DEV * CAP) + src * CAP + r, E * N_DEV * CAP)
    tab = jnp.full((E * N_DEV * CAP,), N_DEV * T, jnp.int32).at[pos].set(tok, mode='drop').reshape(E, N_DEV * CAP)
    gt = jnp.zeros((E * N_DEV * CAP,), jnp.float32).at[pos].set(g.reshape(-1), mode='drop').reshape(E, N_DEV * CAP)

    def step(y, inp):
        t, gw, a1, a3, a2 = inp
        xe = jnp.take(x, t, axis=0, mode='fill', fill_value=0)
        a = jnp.dot(xe, a1, preferred_element_type=jnp.float32)
        b = jnp.dot(xe, a3, preferred_element_type=jnp.float32)
        h = (jax.nn.silu(a) * b).astype(jnp.bfloat16)
        o = jnp.dot(h, a2, preferred_element_type=jnp.float32).astype(jnp.bfloat16)
        return y.at[t].add(gw[:, None] * o.astype(jnp.float32), mode='drop'), None

    y, _ = lax.scan(step, jnp.zeros((N_DEV * T, D), jnp.float32), (tab, gt, w1, w3, w2))
    return y.astype(jnp.bfloat16)
```

```python
import functools

import jax
import jax.numpy as jnp
from jax import lax
from jax.experimental import pallas as pl
from jax.experimental.pallas import tpu as pltpu
from jax.sharding import PartitionSpec as P

MESH = pl.DeviceIdType.MESH
PIECES = 4


def _gate(x, wr, idx):
    logits = jnp.dot(x, wr, preferred_element_type=jnp.float32)
    oh = idx[:, :, None] == jnp.arange(wr.shape[1], dtype=idx.dtype)
    return jax.nn.softmax(jnp.sum(jnp.where(oh, logits[:, None, :], 0.0), axis=-1), axis=-1)


def _kernel(C, B, x_ref, rt_ref, mt_ref, w1_ref, w3_ref, w2_ref, y_ref, o_ref,
            xt, big, sel, hb, ob, w1b, w3b, w2b, wm, part, recv,
            xsem, w1sem, w3sem, w2sem, lsem, xs, xr, osem, ssem, rsem, credit):
    T, D = y_ref.shape
    EL, FF = w2_ref.shape[0], w2_ref.shape[1]
    TH = T // 2
    RP = TH // PIECES
    NF, ND = FF // B, D // B
    z0 = lax.axis_index('outer')
    e0 = lax.axis_index('expert')
    c = lax.rem(e0, 2)
    y0 = e0 // 2
    r = z0 + y0 * (7 - 2 * z0)

    def place(q):
        y = q // 4
        return q + y * (7 - 2 * q), y

    def dev(q):
        z, y = place(q)
        return {'outer': z, 'expert': y * 2 + c}

    nxt = (dev(lax.rem(r + 1, 8)), dev(lax.rem(r + 7, 8)))
    prv = (nxt[1], nxt[0])
    partner = {'outer': z0, 'expert': y0 * 2 + 1 - c}

    def ds(i, n):
        return pl.ds(pl.multiple_of(i * n, n), n)

    def w1_copy(e, cc):
        return pltpu.make_async_copy(w1_ref.at[e, :, ds(cc, B)], w1b.at[cc], w1sem.at[cc])

    def w3_copy(e, cc):
        return pltpu.make_async_copy(w3_ref.at[e, :, ds(cc, B)], w3b.at[cc], w3sem.at[cc])

    def w2_copy(e, nn):
        return pltpu.make_async_copy(w2_ref.at[e, :, ds(nn, B)], w2b.at[nn], w2sem.at[nn])

    for cc in range(NF):
        w1_copy(0, cc).start()
        w3_copy(0, cc).start()
    for nn in range(ND):
        w2_copy(0, nn).start()

    barrier = pltpu.get_barrier_semaphore()
    for d in (*nxt, partner):
        pl.semaphore_signal(barrier, inc=1, device_id=d, device_id_type=MESH)
    pl.semaphore_wait(barrier, 3)

    def chip(j):
        return lax.rem(r - j + 8, 8)

    def ffn(k):
        j0 = k
        j1 = lax.rem(8 - k + 4 * (k // 4), 8)

        def jof(s):
            return j0 + lax.rem(s, 2) * (j1 - j0)

        def src(s):
            z, y = place(chip(jof(s)))
            return z * 4 + y * 2 + c + (s // 2) * (1 - 2 * c)

        def x_copy(s):
            return pltpu.make_async_copy(
                x_ref.at[ds(src(s), T), :], xt.at[lax.rem(s, 2)], xsem.at[lax.rem(s, 2)])

        x_copy(jnp.int32(0)).start()

        def dispatch(s, _):
            @pl.when(s < 3)
            def _():
                x_copy(s + 1).start()

            rt = rt_ref[src(s)]
            io = lax.broadcasted_iota(jnp.int32, (C, T), 0).astype(jnp.float32)
            for e in range(EL):
                sel[e * C:(e + 1) * C, :] = jnp.where(rt[e:e + 1, :] == io, 1.0, 0.0).astype(jnp.bfloat16)
            x_copy(s).wait()

            def body(nn, _):
                v = jnp.dot(sel[...], xt[lax.rem(s, 2), :, ds(nn, B)], preferred_element_type=jnp.float32)
                v = v.astype(jnp.bfloat16)
                for e in range(EL):
                    big[pl.ds(pl.multiple_of(e * 4 * C + s * C, C), C), ds(nn, B)] = v[e * C:(e + 1) * C]
                return 0

            lax.fori_loop(0, ND, body, 0)
            return 0

        lax.fori_loop(0, 4, dispatch, 0)

        def local_copy(e, s):
            return pltpu.make_async_copy(
                ob.at[lax.rem(e, 2), pl.ds(s * C, C)], o_ref.at[jof(s), ds(c * EL + e, C)], lsem.at[e, s])

        def partner_copy(e, s):
            return pltpu.make_async_remote_copy(
                src_ref=ob.at[lax.rem(e, 2), pl.ds((2 + s) * C, C)],
                dst_ref=o_ref.at[jof(s), ds(c * EL + e, C)],
                send_sem=xs.at[e, s], recv_sem=xr.at[k - 1, e, s],
                device_id=partner, device_id_type=MESH)

        def arrival(e, s):
            return pltpu.make_async_remote_copy(
                src_ref=ob.at[lax.rem(e, 2), pl.ds((2 + s) * C, C)],
                dst_ref=o_ref.at[jof(s), ds((1 - c) * EL + e, C)],
                send_sem=xs.at[e, s], recv_sem=xr.at[k - 1, e, s],
                device_id=partner, device_id_type=MESH)

        def expert(e, _):
            more = (k - 1) * EL + e < 4 * EL - 1
            ne = lax.rem(e + 1, EL)

            def up(cc, _):
                w1_copy(e, cc).wait()
                w3_copy(e, cc).wait()
                xe = big[ds(e, 4 * C), :]
                a = jnp.dot(xe, w1b[cc], preferred_element_type=jnp.float32)
                b = jnp.dot(xe, w3b[cc], preferred_element_type=jnp.float32)
                hb[:, ds(cc, B)] = (jax.nn.silu(a) * b).astype(jnp.bfloat16)

                @pl.when(more)
                def _():
                    w1_copy(ne, cc).start()
                    w3_copy(ne, cc).start()

                return 0

            lax.fori_loop(0, NF, up, 0)

            @pl.when(e >= 2)
            def _():
                for s in range(2):
                    local_copy(e - 2, s).wait()
                    partner_copy(e - 2, s).wait_send()

            def down(nn, _):
                w2_copy(e, nn).wait()
                v = jnp.dot(hb[...], w2b[nn], preferred_element_type=jnp.float32)
                ob[lax.rem(e, 2), :, ds(nn, B)] = v.astype(jnp.bfloat16)

                @pl.when(more)
                def _():
                    w2_copy(ne, nn).start()

                return 0

            lax.fori_loop(0, ND, down, 0)
            for s in range(2):
                partner_copy(e, s).start()
                local_copy(e, s).start()
            return 0

        lax.fori_loop(0, EL, expert, 0)
        for e in range(EL):
            for s in range(2):
                if e >= EL - 2:
                    local_copy(e, s).wait()
                    partner_copy(e, s).wait_send()
                arrival(e, s).wait_recv()

    def send(slot, d, p):
        return pltpu.make_async_remote_copy(
            src_ref=part.at[slot, d, ds(p, RP)], dst_ref=recv.at[slot, d, ds(p, RP)],
            send_sem=ssem.at[slot, d, p], recv_sem=rsem.at[slot, d, p],
            device_id=nxt[d], device_id_type=MESH)

    def step(k, _):
        slot = lax.rem(k, 2)
        old = 1 - slot

        @pl.when(k <= 4)
        def _():
            ffn(k)

        @pl.when(k >= 3)
        def _():
            for d in range(2):
                for p in range(PIECES):
                    send(slot, d, p).wait_send()

        def jc(d):
            return lax.rem(k + d * (8 - 2 * k) + 8, 8)

        def o_copy(d):
            return pltpu.make_async_copy(o_ref.at[jc(d)], big.at[ds(d, 8 * C)], osem.at[d])

        o_copy(0).start()
        o_copy(1).start()

        def combine(d, _):
            z, y = place(chip(jc(d)))
            m = mt_ref[z * 2 + y, ds(d, TH), :]
            io = lax.broadcasted_iota(jnp.int32, (TH, C), 1).astype(jnp.float32)
            for e in range(2 * EL):
                w = jnp.where(io == m[:, e:e + 1], m[:, 2 * EL + e:2 * EL + e + 1], 0.0)
                hi = w.astype(jnp.bfloat16)
                w = w - hi.astype(jnp.float32)
                mid = w.astype(jnp.bfloat16)
                lo = (w - mid.astype(jnp.float32)).astype(jnp.bfloat16)
                wm[0:TH, e * C:(e + 1) * C] = hi
                wm[TH:2 * TH, e * C:(e + 1) * C] = mid
                wm[2 * TH:, e * C:(e + 1) * C] = lo
            o_copy(d).wait()

            def body(nn, _):
                v = jnp.dot(wm[...], big[ds(d, 8 * C), ds(nn, B)], preferred_element_type=jnp.float32)
                part[slot, d, :, ds(nn, B)] = v[:TH] + v[TH:2 * TH] + v[2 * TH:]
                return 0

            lax.fori_loop(0, ND, body, 0)
            return 0

        lax.fori_loop(0, 2, combine, 0)

        @pl.when((k >= 3) & (k <= 7))
        def _():
            for d in range(2):
                pl.semaphore_wait(credit.at[d], 1)

        def piece(p, _):
            for d in range(2):
                @pl.when(k >= 2)
                def _():
                    send(old, d, p).wait_recv()

                    @pl.when(k <= 7)
                    def _():
                        part[slot, d, ds(p, RP), :] += recv[old, d, ds(p, RP), :]

                    @pl.when(k == 8)
                    def _():
                        v = part[slot, d, ds(p, RP), :] + recv[old, d, ds(p, RP), :]
                        y_ref[ds(d * PIECES + p, RP), :] = v.astype(y_ref.dtype)

                @pl.when(k <= 7)
                def _():
                    send(slot, d, p).start()

            return 0

        lax.fori_loop(0, PIECES, piece, 0)

        @pl.when((k >= 2) & (k <= 6))
        def _():
            for d in range(2):
                pl.semaphore_signal(credit.at[d], inc=1, device_id=prv[d], device_id_type=MESH)

        return 0

    lax.fori_loop(1, 9, step, 0)
    for d in range(2):
        for p in range(PIECES):
            send(1, d, p).wait_send()


def _experts(x, rt, mt, w1, w3, w2, T, C):
    EL, D, FF = w1.shape
    B = min(256, FF, D)
    TH = T // 2
    bf, f32 = jnp.bfloat16, jnp.float32
    hbm = pl.BlockSpec(memory_space=pl.ANY)
    vmem = pl.BlockSpec(memory_space=pltpu.VMEM)
    dma = pltpu.SemaphoreType.DMA
    flops = 2 * 16 * EL * C * D * (3 * FF + T) + 2 * 16 * EL * C * D * 3 * T
    return pl.pallas_call(
        functools.partial(_kernel, C, B),
        out_shape=(jax.ShapeDtypeStruct((T, D), bf), jax.ShapeDtypeStruct((8, 2 * EL * C, D), bf)),
        in_specs=[hbm, vmem, vmem, hbm, hbm, hbm],
        out_specs=(vmem, hbm),
        scratch_shapes=[
            pltpu.VMEM((2, T, D), bf),
            pltpu.VMEM((16 * C, D), bf),
            pltpu.VMEM((EL * C, T), bf),
            pltpu.VMEM((4 * C, FF), bf),
            pltpu.VMEM((2, 4 * C, D), bf),
            pltpu.VMEM((FF // B, D, B), bf),
            pltpu.VMEM((FF // B, D, B), bf),
            pltpu.VMEM((D // B, FF, B), bf),
            pltpu.VMEM((3 * TH, 2 * EL * C), bf),
            pltpu.VMEM((2, 2, TH, D), f32),
            pltpu.VMEM((2, 2, TH, D), f32),
            dma((2,)), dma((FF // B,)), dma((FF // B,)), dma((D // B,)),
            dma((EL, 2)), dma((EL, 2)), dma((4, EL, 2)), dma((2,)),
            dma((2, 2, PIECES)), dma((2, 2, PIECES)),
            pltpu.SemaphoreType.REGULAR((2,)),
        ],
        compiler_params=pltpu.CompilerParams(
            collective_id=0, has_side_effects=True, vmem_limit_bytes=67043328),
        cost_estimate=pl.CostEstimate(flops=flops, bytes_accessed=400_000_000, transcendentals=0),
    )(x, rt, mt, w1, w3, w2)[0]


def solution(mesh):
    tok = P(('data', 'outer', 'expert'), None)
    wsp = P(('outer', 'expert'), None, None)
    ax = ('outer', 'expert')

    def local(x, wr, idx, w1, w3, w2):
        T, D = x.shape
        K = idx.shape[1]
        E = wr.shape[1]
        EL = w1.shape[0]
        C = 2 * T * K // E
        xa = lax.all_gather(x, ax, axis=0, tiled=True)
        g = _gate(x, wr, idx)
        meta = jnp.concatenate([idx.astype(jnp.float32).T, g.T], axis=0)
        meta = lax.all_gather(meta, ax, axis=0, tiled=False)
        e0 = lax.axis_index('expert')
        core = lax.rem(e0, 2)
        first = (lax.axis_index('outer') * 4 + e0 - core) * EL
        mine = (first + jnp.arange(2 * EL)).astype(jnp.float32)
        oh = meta[:, None, :K, :] == mine[None, :, None, None]
        m = jnp.any(oh, axis=2)
        ge = jnp.sum(jnp.where(oh, meta[:, None, K:, :], 0.0), axis=2)
        pos = jnp.arange(T, dtype=jnp.int32)
        tri = (pos[:, None] < pos[None, :]).astype(jnp.bfloat16)
        cnt = jnp.dot(m.astype(jnp.bfloat16).reshape(-1, T), tri, preferred_element_type=jnp.float32)
        rank = jnp.where(m, cnt.reshape(m.shape), -1.0)
        rt = lax.dynamic_slice_in_dim(rank, core * EL, EL, axis=1)
        mt = jnp.concatenate([rank, ge], axis=1).reshape(8, 2, 4 * EL, T)
        mt = lax.dynamic_index_in_dim(mt, core, axis=1, keepdims=False)
        mt = jnp.swapaxes(mt, 1, 2)
        return _experts(xa, rt, mt, w1, w3, w2, T, C)

    return jax.shard_map(local, mesh=mesh, in_specs=(tok, P(None, None), tok, wsp, wsp, wsp), out_specs=tok, check_vma=False)
```

```python
import functools

import jax
import jax.numpy as jnp
from jax import lax
from jax.experimental import pallas as pl
from jax.experimental.pallas import tpu as pltpu
from jax.sharding import PartitionSpec as P

MESH = pl.DeviceIdType.MESH
PIECES = 4


def _kernel(C, B, x_ref, m_ref, w1_ref, w3_ref, w2_ref, y_ref, o_ref, xa,
            xt, big, sel, hb, ob, w1b, w3b, w2b, wm, part, recv, ma, tm,
            xsem, w1sem, w3sem, w2sem, lsem, xs, xr, osem, ssem, rsem,
            ags, agr, pxs, pxr, pos, por, credit):
    T, D = y_ref.shape
    EL, FF = w2_ref.shape[0], w2_ref.shape[1]
    TH = T // 2
    RP = TH // PIECES
    NF, ND = FF // B, D // B
    z0 = lax.axis_index('outer')
    e0 = lax.axis_index('expert')
    c = lax.rem(e0, 2)
    y0 = e0 // 2
    r = z0 + y0 * (7 - 2 * z0)

    def place(q):
        y = q // 4
        return q + y * (7 - 2 * q), y

    def dev(q):
        z, y = place(q)
        return {'outer': z, 'expert': y * 2 + c}

    nxt = (dev(lax.rem(r + 1, 8)), dev(lax.rem(r + 7, 8)))
    prv = (nxt[1], nxt[0])
    partner = {'outer': z0, 'expert': y0 * 2 + 1 - c}

    def ds(i, n):
        return pl.ds(pl.multiple_of(i * n, n), n)

    def w1_copy(e, cc):
        return pltpu.make_async_copy(w1_ref.at[e, :, ds(cc, B)], w1b.at[cc], w1sem.at[cc])

    def w3_copy(e, cc):
        return pltpu.make_async_copy(w3_ref.at[e, :, ds(cc, B)], w3b.at[cc], w3sem.at[cc])

    def w2_copy(e, nn):
        return pltpu.make_async_copy(w2_ref.at[e, :, ds(nn, B)], w2b.at[nn], w2sem.at[nn])

    for cc in range(NF):
        w1_copy(0, cc).start()
        w3_copy(0, cc).start()
    for nn in range(ND):
        w2_copy(0, nn).start()

    barrier = pltpu.get_barrier_semaphore()
    for d in (*nxt, partner):
        pl.semaphore_signal(barrier, inc=1, device_id=d, device_id_type=MESH)
    pl.semaphore_wait(barrier, 3)

    half = (ds(0, TH), ds(1, TH))
    always = ((0, 0), (1, 1), (0, 2))
    mine = (z0 * 4 + e0) * EL
    base = (z0 * 4 + y0 * 2) * EL

    def jd(k, d):
        return k if d == 0 else 8 - k

    def block(k, d, h, core):
        if h == 2:
            return ma.at[jd(k, d), core]
        return xa.at[jd(k, d), core, half[h]]

    def gather(k, d, h, first=False):
        if first:
            src = m_ref if h == 2 else x_ref.at[half[h]]
        else:
            src = block(k - 1, d, h, c)
        return pltpu.make_async_remote_copy(
            src_ref=src, dst_ref=block(k, d, h, c), send_sem=ags.at[k - 1, d, h], recv_sem=agr.at[k - 1, d, h],
            device_id=nxt[d], device_id_type=MESH)

    def landed(k, d, h):
        return pltpu.make_async_remote_copy(
            src_ref=block(k, d, h, c), dst_ref=block(k, d, h, c), send_sem=ags.at[k - 1, d, h],
            recv_sem=agr.at[k - 1, d, h], device_id=nxt[d], device_id_type=MESH)

    def push(k, d, h, core):
        return pltpu.make_async_remote_copy(
            src_ref=block(k, d, h, core), dst_ref=block(k, d, h, core), send_sem=pxs.at[k - 1, d, h],
            recv_sem=pxr.at[k - 1, d, h], device_id=partner, device_id_type=MESH)

    def own(h, core):
        return pltpu.make_async_remote_copy(
            src_ref=(x_ref, m_ref)[h], dst_ref=(xa, ma)[h].at[0, core], send_sem=pos.at[h], recv_sem=por.at[h],
            device_id=partner, device_id_type=MESH)

    def each(k, last, f):
        for d in range(2):
            for h in range(3):
                pl.when(k <= (last if (d, h) in always else last - 1))(functools.partial(f, d, h))

    def arrive(k):
        def one(d, h):
            landed(k, d, h).wait_recv()
            push(k, d, h, c).start()

            @pl.when(k <= (3 if (d, h) in always else 2))
            def _():
                gather(k + 1, d, h).start()

        each(k, 4, one)

    for h in (2, 0, 1):
        for d in range(2):
            gather(1, d, h, True).start()
    own(0, c).start()
    own(1, c).start()
    ma[0, c] = m_ref[...]
    arrive(jnp.int32(1))

    def chip(j):
        return lax.rem(r - j + 8, 8)

    def table(m, e):
        hit = m[0:8] == e.astype(jnp.float32)
        rank = jnp.sum(jnp.where(hit, m[8:16] + 1.0, 0.0), axis=0, keepdims=True) - 1.0
        return hit, rank

    def ffn(k):
        j0 = k
        j1 = lax.rem(8 - k + 4 * (k // 4), 8)

        def jof(s):
            return j0 + lax.rem(s, 2) * (j1 - j0)

        def core(s):
            return c + (s // 2) * (1 - 2 * c)

        def x_copy(s):
            return pltpu.make_async_copy(
                xa.at[jof(s), core(s)], xt.at[lax.rem(s, 2)], xsem.at[lax.rem(s, 2)])

        def x_start(s):
            local = (k == 4) & (s == 1)

            @pl.when(local)
            def _():
                pltpu.make_async_copy(x_ref, xt.at[lax.rem(s, 2)], xsem.at[lax.rem(s, 2)]).start()

            @pl.when(jnp.logical_not(local))
            def _():
                x_copy(s).start()

        x_start(jnp.int32(0))
        each(k, 4, lambda d, h: push(k, d, h, 1 - c).wait_recv())

        @pl.when(k == 4)
        def _():
            own(0, 1 - c).wait_recv()
            own(1, 1 - c).wait_recv()


        def dispatch(s, _):
            @pl.when(s < 3)
            def _():
                x_start(s + 1)

            m = ma[jof(s), core(s)]
            io = lax.broadcasted_iota(jnp.int32, (C, T), 0).astype(jnp.float32)
            for e in range(EL):
                rank = table(m, mine + e)[1]
                sel[e * C:(e + 1) * C, :] = jnp.where(rank == io, 1.0, 0.0).astype(jnp.bfloat16)
            x_copy(s).wait()

            def body(nn, _):
                v = jnp.dot(sel[...], xt[lax.rem(s, 2), :, ds(nn, B)], preferred_element_type=jnp.float32)
                v = v.astype(jnp.bfloat16)
                for e in range(EL):
                    big[pl.ds(pl.multiple_of(e * 4 * C + s * C, C), C), ds(nn, B)] = v[e * C:(e + 1) * C]
                return 0

            lax.fori_loop(0, ND, body, 0)
            return 0

        lax.fori_loop(0, 4, dispatch, 0)

        def local_copy(e, s):
            return pltpu.make_async_copy(
                ob.at[lax.rem(e, 2), pl.ds(s * C, C)], o_ref.at[jof(s), ds(c * EL + e, C)], lsem.at[e, s])

        def partner_copy(e, s):
            return pltpu.make_async_remote_copy(
                src_ref=ob.at[lax.rem(e, 2), pl.ds((2 + s) * C, C)],
                dst_ref=o_ref.at[jof(s), ds(c * EL + e, C)],
                send_sem=xs.at[e, s], recv_sem=xr.at[k - 1, e, s],
                device_id=partner, device_id_type=MESH)

        def arrival(e, s):
            return pltpu.make_async_remote_copy(
                src_ref=ob.at[lax.rem(e, 2), pl.ds((2 + s) * C, C)],
                dst_ref=o_ref.at[jof(s), ds((1 - c) * EL + e, C)],
                send_sem=xs.at[e, s], recv_sem=xr.at[k - 1, e, s],
                device_id=partner, device_id_type=MESH)

        def expert(e, _):
            more = (k - 1) * EL + e < 4 * EL - 1
            ne = lax.rem(e + 1, EL)

            def up(cc, _):
                w1_copy(e, cc).wait()
                w3_copy(e, cc).wait()
                xe = big[ds(e, 4 * C), :]
                a = jnp.dot(xe, w1b[cc], preferred_element_type=jnp.float32)
                b = jnp.dot(xe, w3b[cc], preferred_element_type=jnp.float32)
                hb[:, ds(cc, B)] = (jax.nn.silu(a) * b).astype(jnp.bfloat16)

                @pl.when(more)
                def _():
                    w1_copy(ne, cc).start()
                    w3_copy(ne, cc).start()

                return 0

            lax.fori_loop(0, NF, up, 0)

            @pl.when((e == 2) & (k <= 3))
            def _():
                arrive(k + 1)

            @pl.when(e >= 2)
            def _():
                for s in range(2):
                    local_copy(e - 2, s).wait()
                    partner_copy(e - 2, s).wait_send()

            def down(nn, _):
                w2_copy(e, nn).wait()
                v = jnp.dot(hb[...], w2b[nn], preferred_element_type=jnp.float32)
                ob[lax.rem(e, 2), :, ds(nn, B)] = v.astype(jnp.bfloat16)

                @pl.when(more)
                def _():
                    w2_copy(ne, nn).start()

                return 0

            lax.fori_loop(0, ND, down, 0)
            for s in range(2):
                partner_copy(e, s).start()
                local_copy(e, s).start()
            return 0

        lax.fori_loop(0, EL, expert, 0)
        for e in range(EL):
            for s in range(2):
                if e >= EL - 2:
                    local_copy(e, s).wait()
                    partner_copy(e, s).wait_send()
                arrival(e, s).wait_recv()

    def send(slot, d, p):
        return pltpu.make_async_remote_copy(
            src_ref=part.at[slot, d, ds(p, RP)], dst_ref=recv.at[slot, d, ds(p, RP)],
            send_sem=ssem.at[slot, d, p], recv_sem=rsem.at[slot, d, p],
            device_id=nxt[d], device_id_type=MESH)

    def step(k, _):
        slot = lax.rem(k, 2)
        old = 1 - slot

        @pl.when(k <= 4)
        def _():
            ffn(k)

        @pl.when(k >= 3)
        def _():
            for d in range(2):
                for p in range(PIECES):
                    send(slot, d, p).wait_send()

        def jc(d):
            return lax.rem(k + d * (8 - 2 * k) + 8, 8)

        def o_copy(d):
            return pltpu.make_async_copy(o_ref.at[jc(d)], big.at[ds(d, 8 * C)], osem.at[d])

        o_copy(0).start()
        o_copy(1).start()

        def combine(d, _):
            m = ma[jc(d), c, :, ds(d, TH)]
            for e in range(2 * EL):
                hit, rank = table(m, base + e)
                tm[e:e + 1, :] = rank
                tm[2 * EL + e:2 * EL + e + 1, :] = jnp.sum(jnp.where(hit, m[16:24], 0.0), axis=0, keepdims=True)
            m = tm[...].T
            io = lax.broadcasted_iota(jnp.int32, (TH, C), 1).astype(jnp.float32)
            for e in range(2 * EL):
                w = jnp.where(io == m[:, e:e + 1], m[:, 2 * EL + e:2 * EL + e + 1], 0.0)
                hi = w.astype(jnp.bfloat16)
                w = w - hi.astype(jnp.float32)
                mid = w.astype(jnp.bfloat16)
                lo = (w - mid.astype(jnp.float32)).astype(jnp.bfloat16)
                wm[0:TH, e * C:(e + 1) * C] = hi
                wm[TH:2 * TH, e * C:(e + 1) * C] = mid
                wm[2 * TH:, e * C:(e + 1) * C] = lo
            o_copy(d).wait()

            def body(nn, _):
                v = jnp.dot(wm[...], big[ds(d, 8 * C), ds(nn, B)], preferred_element_type=jnp.float32)
                part[slot, d, :, ds(nn, B)] = v[:TH] + v[TH:2 * TH] + v[2 * TH:]
                return 0

            lax.fori_loop(0, ND, body, 0)
            return 0

        lax.fori_loop(0, 2, combine, 0)

        @pl.when((k >= 3) & (k <= 7))
        def _():
            for d in range(2):
                pl.semaphore_wait(credit.at[d], 1)

        def piece(p, _):
            for d in range(2):
                @pl.when(k >= 2)
                def _():
                    send(old, d, p).wait_recv()

                    @pl.when(k <= 7)
                    def _():
                        part[slot, d, ds(p, RP), :] += recv[old, d, ds(p, RP), :]

                    @pl.when(k == 8)
                    def _():
                        v = part[slot, d, ds(p, RP), :] + recv[old, d, ds(p, RP), :]
                        y_ref[ds(d * PIECES + p, RP), :] = v.astype(y_ref.dtype)

                @pl.when(k <= 7)
                def _():
                    send(slot, d, p).start()

            return 0

        lax.fori_loop(0, PIECES, piece, 0)

        @pl.when((k >= 2) & (k <= 6))
        def _():
            for d in range(2):
                pl.semaphore_signal(credit.at[d], inc=1, device_id=prv[d], device_id_type=MESH)

        return 0

    lax.fori_loop(1, 9, step, 0)
    for d in range(2):
        for p in range(PIECES):
            send(1, d, p).wait_send()

    def drain(k, _):
        each(k, 4, lambda d, h: landed(k, d, h).wait_send())
        each(k, 4, lambda d, h: push(k, d, h, c).wait_send())
        return 0

    lax.fori_loop(1, 5, drain, 0)
    own(0, c).wait_send()
    own(1, c).wait_send()


def _experts(x, meta, w1, w3, w2, C):
    EL, D, FF = w1.shape
    T = x.shape[0]
    B = min(256, FF, D)
    TH = T // 2
    bf, f32 = jnp.bfloat16, jnp.float32
    hbm = pl.BlockSpec(memory_space=pl.ANY)
    vmem = pl.BlockSpec(memory_space=pltpu.VMEM)
    dma = pltpu.SemaphoreType.DMA
    flops = 2 * 16 * EL * C * D * (3 * FF + T) + 2 * 16 * EL * C * D * 3 * T
    return pl.pallas_call(
        functools.partial(_kernel, C, B),
        out_shape=(jax.ShapeDtypeStruct((T, D), bf), jax.ShapeDtypeStruct((8, 2 * EL * C, D), bf),
                   jax.ShapeDtypeStruct((8, 2, T, D), bf)),
        in_specs=[hbm, vmem, hbm, hbm, hbm],
        out_specs=(vmem, hbm, hbm),
        scratch_shapes=[
            pltpu.VMEM((2, T, D), bf),
            pltpu.VMEM((16 * C, D), bf),
            pltpu.VMEM((EL * C, T), bf),
            pltpu.VMEM((4 * C, FF), bf),
            pltpu.VMEM((2, 4 * C, D), bf),
            pltpu.VMEM((FF // B, D, B), bf),
            pltpu.VMEM((FF // B, D, B), bf),
            pltpu.VMEM((D // B, FF, B), bf),
            pltpu.VMEM((3 * TH, 2 * EL * C), bf),
            pltpu.VMEM((2, 2, TH, D), f32),
            pltpu.VMEM((2, 2, TH, D), f32),
            pltpu.VMEM((8, 2, *meta.shape), f32),
            pltpu.VMEM((4 * EL, TH), f32),
            dma((2,)), dma((FF // B,)), dma((FF // B,)), dma((D // B,)),
            dma((EL, 2)), dma((EL, 2)), dma((4, EL, 2)), dma((2,)),
            dma((2, 2, PIECES)), dma((2, 2, PIECES)),
            dma((4, 2, 3)), dma((4, 2, 3)), dma((4, 2, 3)), dma((4, 2, 3)), dma((2,)), dma((2,)),
            pltpu.SemaphoreType.REGULAR((2,)),
        ],
        compiler_params=pltpu.CompilerParams(
            collective_id=0, has_side_effects=True, vmem_limit_bytes=67043328),
        cost_estimate=pl.CostEstimate(flops=flops, bytes_accessed=400_000_000, transcendentals=0),
    )(x, meta, w1, w3, w2)[0]


def solution(mesh):
    tok = P(('data', 'outer', 'expert'), None)
    wsp = P(('outer', 'expert'), None, None)

    def local(x, wr, idx, w1, w3, w2):
        T, D = x.shape
        E = wr.shape[1]
        C = 2 * T * idx.shape[1] // E
        oh = idx[:, :, None] == jnp.arange(E, dtype=idx.dtype)
        logits = jnp.dot(x, wr, preferred_element_type=jnp.float32)
        g = jax.nn.softmax(jnp.sum(jnp.where(oh, logits[:, None, :], 0.0), axis=-1), axis=-1)
        pos = jnp.arange(T, dtype=jnp.int32)
        tri = (pos[None, :] < pos[:, None]).astype(jnp.bfloat16)
        cnt = jnp.dot(tri, jnp.any(oh, axis=1).astype(jnp.bfloat16), preferred_element_type=jnp.float32)
        rank = jnp.sum(jnp.where(oh, cnt[:, None, :], 0.0), axis=-1)
        meta = jnp.concatenate([idx.astype(jnp.float32), rank, g], axis=1).T
        return _experts(x, meta, w1, w3, w2, C)

    return jax.shard_map(local, mesh=mesh, in_specs=(tok, P(None, None), tok, wsp, wsp, wsp), out_specs=tok, check_vma=False)
```

```python
import functools

import jax
import jax.numpy as jnp
from jax import lax
from jax.experimental import pallas as pl
from jax.experimental.pallas import tpu as pltpu
from jax.sharding import PartitionSpec as P

MESH = pl.DeviceIdType.MESH
PIECES = 4


def _kernel(C, B, x_ref, i_ref, wr_ref, w1_ref, w3_ref, w2_ref, y_ref, o_ref, xa,
            xt, big, sel, hb, ob, w1b, w3b, w2b, wm, part, recv, ma, tm, mv,
            xsem, w1sem, w3sem, w2sem, lsem, xs, xr, osem, ssem, rsem,
            ags, agr, pxs, pxr, pos, por, credit):
    T, D = y_ref.shape
    EL, FF = w2_ref.shape[0], w2_ref.shape[1]
    TH = T // 2
    RP = TH // PIECES
    NF, ND = FF // B, D // B
    z0 = lax.axis_index('outer')
    e0 = lax.axis_index('expert')
    c = lax.rem(e0, 2)
    y0 = e0 // 2
    r = z0 + y0 * (7 - 2 * z0)

    def place(q):
        y = q // 4
        return q + y * (7 - 2 * q), y

    def dev(q):
        z, y = place(q)
        return {'outer': z, 'expert': y * 2 + c}

    nxt = (dev(lax.rem(r + 1, 8)), dev(lax.rem(r + 7, 8)))
    prv = (nxt[1], nxt[0])
    partner = {'outer': z0, 'expert': y0 * 2 + 1 - c}

    def ds(i, n):
        return pl.ds(pl.multiple_of(i * n, n), n)

    def w1_copy(e, cc):
        return pltpu.make_async_copy(w1_ref.at[e, :, ds(cc, B)], w1b.at[cc], w1sem.at[cc])

    def w3_copy(e, cc):
        return pltpu.make_async_copy(w3_ref.at[e, :, ds(cc, B)], w3b.at[cc], w3sem.at[cc])

    def w2_copy(e, nn):
        return pltpu.make_async_copy(w2_ref.at[e, :, ds(nn, B)], w2b.at[nn], w2sem.at[nn])

    xload = pltpu.make_async_copy(x_ref, xt.at[0], xsem.at[0])
    xload.start()
    for cc in range(NF):
        w1_copy(0, cc).start()
        w3_copy(0, cc).start()
    for nn in range(ND):
        w2_copy(0, nn).start()

    barrier = pltpu.get_barrier_semaphore()
    for d in (*nxt, partner):
        pl.semaphore_signal(barrier, inc=1, device_id=d, device_id_type=MESH)
    pl.semaphore_wait(barrier, 3)

    half = (ds(0, TH), ds(1, TH))
    always = ((0, 0), (1, 1), (0, 2))
    mine = (z0 * 4 + e0) * EL
    base = (z0 * 4 + y0 * 2) * EL

    def jd(k, d):
        return k if d == 0 else 8 - k

    def block(k, d, h, core):
        if h == 2:
            return ma.at[jd(k, d), core]
        return xa.at[jd(k, d), core, half[h]]

    def gather(k, d, h, first=False):
        if first:
            src = mv if h == 2 else x_ref.at[half[h]]
        else:
            src = block(k - 1, d, h, c)
        return pltpu.make_async_remote_copy(
            src_ref=src, dst_ref=block(k, d, h, c), send_sem=ags.at[k - 1, d, h], recv_sem=agr.at[k - 1, d, h],
            device_id=nxt[d], device_id_type=MESH)

    def landed(k, d, h):
        return pltpu.make_async_remote_copy(
            src_ref=block(k, d, h, c), dst_ref=block(k, d, h, c), send_sem=ags.at[k - 1, d, h],
            recv_sem=agr.at[k - 1, d, h], device_id=nxt[d], device_id_type=MESH)

    def push(k, d, h, core):
        return pltpu.make_async_remote_copy(
            src_ref=block(k, d, h, core), dst_ref=block(k, d, h, core), send_sem=pxs.at[k - 1, d, h],
            recv_sem=pxr.at[k - 1, d, h], device_id=partner, device_id_type=MESH)

    def own(h, core):
        return pltpu.make_async_remote_copy(
            src_ref=(x_ref, mv)[h], dst_ref=(xa, ma)[h].at[0, core], send_sem=pos.at[h], recv_sem=por.at[h],
            device_id=partner, device_id_type=MESH)

    def each(k, last, f):
        for d in range(2):
            for h in range(3):
                pl.when(k <= (last if (d, h) in always else last - 1))(functools.partial(f, d, h))

    def arrive(k):
        def one(d, h):
            landed(k, d, h).wait_recv()
            push(k, d, h, c).start()

            @pl.when(k <= (3 if (d, h) in always else 2))
            def _():
                gather(k + 1, d, h).start()

        each(k, 4, one)

    def chip(j):
        return lax.rem(r - j + 8, 8)

    def table(m, e):
        hit = m[0:8] == e.astype(jnp.float32)
        rank = jnp.sum(jnp.where(hit, m[8:16] + 1.0, 0.0), axis=0, keepdims=True) - 1.0
        return hit, rank

    def route():
        E = wr_ref.shape[0]
        ix = i_ref[...]
        logits = lax.dot_general(wr_ref[...], xt[0], (((1,), (1,)), ((), ())), preferred_element_type=jnp.float32)
        ids = lax.broadcasted_iota(jnp.int32, (E, T), 0)
        got = [jnp.sum(jnp.where(ids == ix[j:j + 1], logits, 0.0), axis=0, keepdims=True) for j in range(8)]
        top = functools.reduce(jnp.maximum, got)
        got = [jnp.exp(v - top) for v in got]
        total = functools.reduce(jnp.add, got)
        used = functools.reduce(jnp.logical_or, [ids == ix[j:j + 1] for j in range(8)])
        before = lax.broadcasted_iota(jnp.int32, (T, T), 0) < lax.broadcasted_iota(jnp.int32, (T, T), 1)
        cnt = jnp.dot(jnp.where(used, 1.0, 0.0).astype(jnp.bfloat16), jnp.where(before, 1.0, 0.0).astype(jnp.bfloat16),
                      preferred_element_type=jnp.float32)
        mv[0:8, :] = ix.astype(jnp.float32)
        for j in range(8):
            mv[8 + j:9 + j, :] = jnp.sum(jnp.where(ids == ix[j:j + 1], cnt, 0.0), axis=0, keepdims=True)
            mv[16 + j:17 + j, :] = got[j] / total

    def ffn(k, S):
        k = jnp.int32(k)
        n = 2 * S
        j0 = k
        j1 = 8 - k if S == 2 else k

        def jof(s):
            return j0 + lax.rem(s, S) * (j1 - j0)

        def core(s):
            return c + (s // S) * (1 - 2 * c)

        def x_start(s):
            pltpu.make_async_copy(xa.at[jof(s), core(s)], xt.at[lax.rem(s, 2)], xsem.at[lax.rem(s, 2)]).start()

        def x_wait(s):
            pltpu.make_async_copy(x_ref, xt.at[lax.rem(s, 2)], xsem.at[lax.rem(s, 2)]).wait()

        def dispatch(s, _):
            @pl.when(s < n - 1)
            def _():
                x_start(s + 1)

            m = ma[jof(s), core(s)]
            io = lax.broadcasted_iota(jnp.int32, (C, T), 0).astype(jnp.float32)
            for e in range(EL):
                rank = table(m, mine + e)[1]
                sel[e * C:(e + 1) * C, :] = jnp.where(rank == io, 1.0, 0.0).astype(jnp.bfloat16)

            @pl.when((k > 0) | (s > 0))
            def _():
                x_wait(s)

            def body(nn, _):
                v = jnp.dot(sel[...], xt[lax.rem(s, 2), :, ds(nn, B)], preferred_element_type=jnp.float32)
                v = v.astype(jnp.bfloat16)
                for e in range(EL):
                    big[pl.ds(pl.multiple_of(e * n * C + s * C, C), C), ds(nn, B)] = v[e * C:(e + 1) * C]
                return 0

            lax.fori_loop(0, ND, body, 0)
            return 0

        def start_first():
            x_start(jnp.int32(0))
            each(k, 4, lambda d, h: push(k, d, h, 1 - c).wait_recv())

        if S == 2:
            start_first()
        else:
            pl.when(k > 0)(start_first)

            @pl.when(k == 0)
            def _():
                own(0, 1 - c).wait_recv()
                own(1, 1 - c).wait_recv()

        lax.fori_loop(0, n, dispatch, 0)

        def local_copy(e, s):
            return pltpu.make_async_copy(
                ob.at[lax.rem(e, 2), pl.ds(s * C, C)], o_ref.at[jof(s), ds(c * EL + e, C)], lsem.at[e, s])

        def partner_copy(e, s):
            return pltpu.make_async_remote_copy(
                src_ref=ob.at[lax.rem(e, 2), pl.ds((S + s) * C, C)],
                dst_ref=o_ref.at[jof(s), ds(c * EL + e, C)],
                send_sem=xs.at[e, s], recv_sem=xr.at[k, e, s],
                device_id=partner, device_id_type=MESH)

        def arrival(e, s):
            return pltpu.make_async_remote_copy(
                src_ref=ob.at[lax.rem(e, 2), pl.ds((S + s) * C, C)],
                dst_ref=o_ref.at[jof(s), ds((1 - c) * EL + e, C)],
                send_sem=xs.at[e, s], recv_sem=xr.at[k, e, s],
                device_id=partner, device_id_type=MESH)

        def expert(e, _):
            more = k * EL + e < 5 * EL - 1
            ne = lax.rem(e + 1, EL)

            def up(cc, _):
                w1_copy(e, cc).wait()
                w3_copy(e, cc).wait()
                xe = big[ds(e, n * C), :]
                a = jnp.dot(xe, w1b[cc], preferred_element_type=jnp.float32)
                b = jnp.dot(xe, w3b[cc], preferred_element_type=jnp.float32)
                hb[0:n * C, ds(cc, B)] = (jax.nn.silu(a) * b).astype(jnp.bfloat16)

                @pl.when(more)
                def _():
                    w1_copy(ne, cc).start()
                    w3_copy(ne, cc).start()

                return 0

            lax.fori_loop(0, NF, up, 0)

            @pl.when(e >= 2)
            def _():
                for s in range(S):
                    local_copy(e - 2, s).wait()
                    partner_copy(e - 2, s).wait_send()

            def down(nn, _):
                w2_copy(e, nn).wait()
                v = jnp.dot(hb[0:n * C, :], w2b[nn], preferred_element_type=jnp.float32)
                ob[lax.rem(e, 2), 0:n * C, ds(nn, B)] = v.astype(jnp.bfloat16)

                @pl.when(more)
                def _():
                    w2_copy(ne, nn).start()

                return 0

            lax.fori_loop(0, ND, down, 0)
            for s in range(S):
                partner_copy(e, s).start()
                local_copy(e, s).start()
            return 0

        lax.fori_loop(0, EL, expert, 0)
        pl.when(k <= 3)(lambda: arrive(k + 1))
        for e in range(EL):
            for s in range(S):
                if e >= EL - 2:
                    local_copy(e, s).wait()
                    partner_copy(e, s).wait_send()
                arrival(e, s).wait_recv()

    def send(slot, d, p):
        return pltpu.make_async_remote_copy(
            src_ref=part.at[slot, d, ds(p, RP)], dst_ref=recv.at[slot, d, ds(p, RP)],
            send_sem=ssem.at[slot, d, p], recv_sem=rsem.at[slot, d, p],
            device_id=nxt[d], device_id_type=MESH)

    def step(k, _):
        slot = lax.rem(k, 2)
        old = 1 - slot

        pl.when(k <= 3)(lambda: ffn(k, 2))
        pl.when(k == 4)(lambda: ffn(k, 1))

        @pl.when(k >= 3)
        def _():
            for d in range(2):
                for p in range(PIECES):
                    send(slot, d, p).wait_send()

        def jc(d):
            return lax.rem(k + d * (8 - 2 * k) + 8, 8)

        def o_copy(d):
            return pltpu.make_async_copy(o_ref.at[jc(d)], big.at[ds(d, 8 * C)], osem.at[d])

        o_copy(0).start()
        o_copy(1).start()

        def combine(d, _):
            m = ma[jc(d), c, :, ds(d, TH)]
            for e in range(2 * EL):
                hit, rank = table(m, base + e)
                tm[e:e + 1, :] = rank
                tm[2 * EL + e:2 * EL + e + 1, :] = jnp.sum(jnp.where(hit, m[16:24], 0.0), axis=0, keepdims=True)
            m = tm[...].T
            io = lax.broadcasted_iota(jnp.int32, (TH, C), 1).astype(jnp.float32)
            for e in range(2 * EL):
                w = jnp.where(io == m[:, e:e + 1], m[:, 2 * EL + e:2 * EL + e + 1], 0.0)
                hi = w.astype(jnp.bfloat16)
                w = w - hi.astype(jnp.float32)
                mid = w.astype(jnp.bfloat16)
                lo = (w - mid.astype(jnp.float32)).astype(jnp.bfloat16)
                wm[0:TH, e * C:(e + 1) * C] = hi
                wm[TH:2 * TH, e * C:(e + 1) * C] = mid
                wm[2 * TH:, e * C:(e + 1) * C] = lo
            o_copy(d).wait()

            def body(nn, _):
                v = jnp.dot(wm[...], big[ds(d, 8 * C), ds(nn, B)], preferred_element_type=jnp.float32)
                part[slot, d, :, ds(nn, B)] = v[:TH] + v[TH:2 * TH] + v[2 * TH:]
                return 0

            lax.fori_loop(0, ND, body, 0)
            return 0

        lax.fori_loop(0, 2, combine, 0)

        @pl.when((k >= 3) & (k <= 7))
        def _():
            for d in range(2):
                pl.semaphore_wait(credit.at[d], 1)

        def piece(p, _):
            for d in range(2):
                @pl.when(k >= 2)
                def _():
                    send(old, d, p).wait_recv()

                    @pl.when(k <= 7)
                    def _():
                        part[slot, d, ds(p, RP), :] += recv[old, d, ds(p, RP), :]

                    @pl.when(k == 8)
                    def _():
                        v = part[slot, d, ds(p, RP), :] + recv[old, d, ds(p, RP), :]
                        y_ref[ds(d * PIECES + p, RP), :] = v.astype(y_ref.dtype)

                @pl.when(k <= 7)
                def _():
                    send(slot, d, p).start()

            return 0

        lax.fori_loop(0, PIECES, piece, 0)

        @pl.when((k >= 2) & (k <= 6))
        def _():
            for d in range(2):
                pl.semaphore_signal(credit.at[d], inc=1, device_id=prv[d], device_id_type=MESH)

        return 0

    for h in range(2):
        for d in range(2):
            gather(1, d, h, True).start()
    own(0, c).start()
    xload.wait()
    route()
    ma[0, c] = mv[...]
    for d in range(2):
        gather(1, d, 2, True).start()
    own(1, c).start()
    ffn(0, 1)
    lax.fori_loop(1, 9, step, 0)
    for d in range(2):
        for p in range(PIECES):
            send(1, d, p).wait_send()

    def drain(k, _):
        each(k, 4, lambda d, h: landed(k, d, h).wait_send())
        each(k, 4, lambda d, h: push(k, d, h, c).wait_send())
        return 0

    lax.fori_loop(1, 5, drain, 0)
    own(0, c).wait_send()
    own(1, c).wait_send()


def _experts(x, idx, wr, w1, w3, w2, C):
    EL, D, FF = w1.shape
    T = x.shape[0]
    B = min(256, FF, D)
    TH = T // 2
    bf, f32 = jnp.bfloat16, jnp.float32
    hbm = pl.BlockSpec(memory_space=pl.ANY)
    vmem = pl.BlockSpec(memory_space=pltpu.VMEM)
    dma = pltpu.SemaphoreType.DMA
    flops = 2 * 16 * EL * C * D * (3 * FF + T) + 2 * 16 * EL * C * D * 3 * T
    return pl.pallas_call(
        functools.partial(_kernel, C, B),
        out_shape=(jax.ShapeDtypeStruct((T, D), bf), jax.ShapeDtypeStruct((8, 2 * EL * C, D), bf),
                   jax.ShapeDtypeStruct((8, 2, T, D), bf)),
        in_specs=[hbm, vmem, vmem, hbm, hbm, hbm],
        out_specs=(vmem, hbm, hbm),
        scratch_shapes=[
            pltpu.VMEM((2, T, D), bf),
            pltpu.VMEM((16 * C, D), bf),
            pltpu.VMEM((EL * C, T), bf),
            pltpu.VMEM((4 * C, FF), bf),
            pltpu.VMEM((2, 4 * C, D), bf),
            pltpu.VMEM((FF // B, D, B), bf),
            pltpu.VMEM((FF // B, D, B), bf),
            pltpu.VMEM((D // B, FF, B), bf),
            pltpu.VMEM((3 * TH, 2 * EL * C), bf),
            pltpu.VMEM((2, 2, TH, D), f32),
            pltpu.VMEM((2, 2, TH, D), f32),
            pltpu.VMEM((8, 2, 24, T), f32),
            pltpu.VMEM((4 * EL, TH), f32),
            pltpu.VMEM((24, T), f32),
            dma((2,)), dma((FF // B,)), dma((FF // B,)), dma((D // B,)),
            dma((EL, 2)), dma((EL, 2)), dma((5, EL, 2)), dma((2,)),
            dma((2, 2, PIECES)), dma((2, 2, PIECES)),
            dma((4, 2, 3)), dma((4, 2, 3)), dma((4, 2, 3)), dma((4, 2, 3)), dma((2,)), dma((2,)),
            pltpu.SemaphoreType.REGULAR((2,)),
        ],
        compiler_params=pltpu.CompilerParams(
            collective_id=0, has_side_effects=True, vmem_limit_bytes=67043328),
        cost_estimate=pl.CostEstimate(flops=flops, bytes_accessed=400_000_000, transcendentals=0),
    )(x, idx, wr, w1, w3, w2)[0]


def solution(mesh):
    tok = P(('data', 'outer', 'expert'), None)
    wsp = P(('outer', 'expert'), None, None)

    def local(x, wr, idx, w1, w3, w2):
        T, D = x.shape
        C = 2 * T * idx.shape[1] // wr.shape[1]
        return _experts(x, idx.T, wr.T, w1, w3, w2, C)

    return jax.shard_map(local, mesh=mesh, in_specs=(tok, P(None, None), tok, wsp, wsp, wsp), out_specs=tok, check_vma=False)
```

```python
import functools

import jax
import jax.numpy as jnp
from jax import lax
from jax.experimental import pallas as pl
from jax.experimental.pallas import tpu as pltpu
from jax.sharding import PartitionSpec as P

MESH = pl.DeviceIdType.MESH
PIECES = 4


def _kernel(C, B, x_ref, i_ref, wr_ref, w1_ref, w3_ref, w2_ref, y_ref, o_ref, xa,
            xt, big, sel, hb, ob, w1b, w3b, w2b, wm, part, recv, ma, tm, mv,
            xsem, w1sem, w3sem, w2sem, lsem, xs, xr, osem, ssem, rsem,
            ags, agr, pxs, pxr, pos, por, credit):
    T, D = y_ref.shape
    EL, FF = w2_ref.shape[0], w2_ref.shape[1]
    TH = T // 2
    RP = TH // PIECES
    NF, ND = FF // B, D // B
    z0 = lax.axis_index('outer')
    e0 = lax.axis_index('expert')
    c = lax.rem(e0, 2)
    y0 = e0 // 2
    r = z0 + y0 * (7 - 2 * z0)

    def place(q):
        y = q // 4
        return q + y * (7 - 2 * q), y

    def dev(q):
        z, y = place(q)
        return {'outer': z, 'expert': y * 2 + c}

    nxt = (dev(lax.rem(r + 1, 8)), dev(lax.rem(r + 7, 8)))
    prv = (nxt[1], nxt[0])
    partner = {'outer': z0, 'expert': y0 * 2 + 1 - c}

    def ds(i, n):
        return pl.ds(pl.multiple_of(i * n, n), n)

    def w1_copy(e, cc):
        return pltpu.make_async_copy(w1_ref.at[e, :, ds(cc, B)], w1b.at[cc], w1sem.at[cc])

    def w3_copy(e, cc):
        return pltpu.make_async_copy(w3_ref.at[e, :, ds(cc, B)], w3b.at[cc], w3sem.at[cc])

    def w2_copy(e, nn):
        return pltpu.make_async_copy(w2_ref.at[e, :, ds(nn, B)], w2b.at[nn], w2sem.at[nn])

    xload = pltpu.make_async_copy(x_ref, xt.at[0], xsem.at[0])
    xload.start()
    for cc in range(NF):
        w1_copy(0, cc).start()
        w3_copy(0, cc).start()
    for nn in range(ND):
        w2_copy(0, nn).start()

    barrier = pltpu.get_barrier_semaphore()
    for d in (*nxt, partner):
        pl.semaphore_signal(barrier, inc=1, device_id=d, device_id_type=MESH)
    pl.semaphore_wait(barrier, 3)

    half = (ds(0, TH), ds(1, TH))
    always = ((0, 0), (1, 1), (0, 2))
    mine = (z0 * 4 + e0) * EL
    base = (z0 * 4 + y0 * 2) * EL

    def jd(k, d):
        return k if d == 0 else 8 - k

    def block(k, d, h, core):
        if h == 2:
            return ma.at[jd(k, d), core]
        return xa.at[jd(k, d), core, half[h]]

    def gather(k, d, h, first=False):
        if first:
            src = mv if h == 2 else x_ref.at[half[h]]
        else:
            src = block(k - 1, d, h, c)
        return pltpu.make_async_remote_copy(
            src_ref=src, dst_ref=block(k, d, h, c), send_sem=ags.at[k - 1, d, h], recv_sem=agr.at[k - 1, d, h],
            device_id=nxt[d], device_id_type=MESH)

    def landed(k, d, h):
        return pltpu.make_async_remote_copy(
            src_ref=block(k, d, h, c), dst_ref=block(k, d, h, c), send_sem=ags.at[k - 1, d, h],
            recv_sem=agr.at[k - 1, d, h], device_id=nxt[d], device_id_type=MESH)

    def push(k, d, h, core):
        return pltpu.make_async_remote_copy(
            src_ref=block(k, d, h, core), dst_ref=block(k, d, h, core), send_sem=pxs.at[k - 1, d, h],
            recv_sem=pxr.at[k - 1, d, h], device_id=partner, device_id_type=MESH)

    def own(h, core):
        return pltpu.make_async_remote_copy(
            src_ref=(x_ref, mv)[h], dst_ref=(xa, ma)[h].at[0, core], send_sem=pos.at[h], recv_sem=por.at[h],
            device_id=partner, device_id_type=MESH)

    def each(k, last, f):
        for d in range(2):
            for h in range(3):
                pl.when(k <= (last if (d, h) in always else last - 1))(functools.partial(f, d, h))

    def arrive(k):
        def one(d, h):
            landed(k, d, h).wait_recv()
            push(k, d, h, c).start()

            @pl.when(k <= (3 if (d, h) in always else 2))
            def _():
                gather(k + 1, d, h).start()

        each(k, 4, one)

    def chip(j):
        return lax.rem(r - j + 8, 8)

    def table(m, e):
        hit = m[0:8] == e.astype(jnp.float32)
        rank = jnp.sum(jnp.where(hit, m[8:16] + 1.0, 0.0), axis=0, keepdims=True) - 1.0
        return hit, rank

    def route():
        E = wr_ref.shape[0]
        ix = i_ref[...]
        logits = lax.dot_general(wr_ref[...], xt[0], (((1,), (1,)), ((), ())), preferred_element_type=jnp.float32)
        ids = lax.broadcasted_iota(jnp.int32, (E, T), 0)
        got = [jnp.sum(jnp.where(ids == ix[j:j + 1], logits, 0.0), axis=0, keepdims=True) for j in range(8)]
        top = functools.reduce(jnp.maximum, got)
        got = [jnp.exp(v - top) for v in got]
        total = functools.reduce(jnp.add, got)
        used = functools.reduce(jnp.logical_or, [ids == ix[j:j + 1] for j in range(8)])
        before = lax.broadcasted_iota(jnp.int32, (T, T), 0) < lax.broadcasted_iota(jnp.int32, (T, T), 1)
        cnt = jnp.dot(jnp.where(used, 1.0, 0.0).astype(jnp.bfloat16), jnp.where(before, 1.0, 0.0).astype(jnp.bfloat16),
                      preferred_element_type=jnp.float32)
        mv[0:8, :] = ix.astype(jnp.float32)
        for j in range(8):
            mv[8 + j:9 + j, :] = jnp.sum(jnp.where(ids == ix[j:j + 1], cnt, 0.0), axis=0, keepdims=True)
            mv[16 + j:17 + j, :] = got[j] / total

    def ffn(k, S):
        k = jnp.int32(k)
        n = 2 * S
        j0 = k
        j1 = 8 - k if S == 2 else k

        def jof(s):
            return j0 + lax.rem(s, S) * (j1 - j0)

        def core(s):
            return c + (s // S) * (1 - 2 * c)

        def x_start(s):
            pltpu.make_async_copy(xa.at[jof(s), core(s)], xt.at[lax.rem(s, 2)], xsem.at[lax.rem(s, 2)]).start()

        def x_wait(s):
            pltpu.make_async_copy(x_ref, xt.at[lax.rem(s, 2)], xsem.at[lax.rem(s, 2)]).wait()

        def dispatch(s, _):
            @pl.when(s < n - 1)
            def _():
                x_start(s + 1)

            m = ma[jof(s), core(s)]
            io = lax.broadcasted_iota(jnp.int32, (C, T), 0).astype(jnp.float32)
            for e in range(EL):
                rank = table(m, mine + e)[1]
                sel[e * C:(e + 1) * C, :] = jnp.where(rank == io, 1.0, 0.0).astype(jnp.bfloat16)

            @pl.when((k > 0) | (s > 0))
            def _():
                x_wait(s)

            def body(nn, _):
                v = jnp.dot(sel[...], xt[lax.rem(s, 2), :, ds(nn, B)], preferred_element_type=jnp.float32)
                v = v.astype(jnp.bfloat16)
                for e in range(EL):
                    big[pl.ds(pl.multiple_of(e * n * C + s * C, C), C), ds(nn, B)] = v[e * C:(e + 1) * C]
                return 0

            lax.fori_loop(0, ND, body, 0)
            return 0

        def start_first():
            x_start(jnp.int32(0))
            each(k, 4, lambda d, h: push(k, d, h, 1 - c).wait_recv())

        if S == 2:
            start_first()
        else:
            pl.when(k > 0)(start_first)

            @pl.when(k == 0)
            def _():
                own(0, 1 - c).wait_recv()
                own(1, 1 - c).wait_recv()

        lax.fori_loop(0, n, dispatch, 0)

        def local_copy(e, s):
            return pltpu.make_async_copy(
                ob.at[lax.rem(e, 2), pl.ds(s * C, C)], o_ref.at[jof(s), ds(c * EL + e, C)], lsem.at[e, s])

        def partner_copy(e, s):
            return pltpu.make_async_remote_copy(
                src_ref=ob.at[lax.rem(e, 2), pl.ds((S + s) * C, C)],
                dst_ref=o_ref.at[jof(s), ds(c * EL + e, C)],
                send_sem=xs.at[e, s], recv_sem=xr.at[k, e, s],
                device_id=partner, device_id_type=MESH)

        def arrival(e, s):
            return pltpu.make_async_remote_copy(
                src_ref=ob.at[lax.rem(e, 2), pl.ds((S + s) * C, C)],
                dst_ref=o_ref.at[jof(s), ds((1 - c) * EL + e, C)],
                send_sem=xs.at[e, s], recv_sem=xr.at[k, e, s],
                device_id=partner, device_id_type=MESH)

        def expert(e, _):
            more = k * EL + e < 5 * EL - 1
            ne = lax.rem(e + 1, EL)
            if S == 2:
                pl.when(e == EL - 1)(lambda: arrive(k + 1))

            def up(cc, _):
                w1_copy(e, cc).wait()
                w3_copy(e, cc).wait()
                xe = big[ds(e, n * C), :]
                a = jnp.dot(xe, w1b[cc], preferred_element_type=jnp.float32)
                b = jnp.dot(xe, w3b[cc], preferred_element_type=jnp.float32)
                hb[0:n * C, ds(cc, B)] = (jax.nn.silu(a) * b).astype(jnp.bfloat16)

                @pl.when(more)
                def _():
                    w1_copy(ne, cc).start()
                    w3_copy(ne, cc).start()

                return 0

            lax.fori_loop(0, NF, up, 0)

            @pl.when(e >= 2)
            def _():
                for s in range(S):
                    local_copy(e - 2, s).wait()
                    partner_copy(e - 2, s).wait_send()

            def down(nn, _):
                w2_copy(e, nn).wait()
                v = jnp.dot(hb[0:n * C, :], w2b[nn], preferred_element_type=jnp.float32)
                ob[lax.rem(e, 2), 0:n * C, ds(nn, B)] = v.astype(jnp.bfloat16)

                @pl.when(more)
                def _():
                    w2_copy(ne, nn).start()

                return 0

            lax.fori_loop(0, ND, down, 0)
            for s in range(S):
                partner_copy(e, s).start()
                local_copy(e, s).start()
            return 0

        lax.fori_loop(0, EL, expert, 0)
        if S == 1:
            pl.when(k == 0)(lambda: arrive(k + 1))
        for e in range(EL):
            for s in range(S):
                if e >= EL - 2:
                    local_copy(e, s).wait()
                    partner_copy(e, s).wait_send()
                arrival(e, s).wait_recv()

    def send(slot, d, p):
        return pltpu.make_async_remote_copy(
            src_ref=part.at[slot, d, ds(p, RP)], dst_ref=recv.at[slot, d, ds(p, RP)],
            send_sem=ssem.at[slot, d, p], recv_sem=rsem.at[slot, d, p],
            device_id=nxt[d], device_id_type=MESH)

    def step(k, _):
        slot = lax.rem(k, 2)
        old = 1 - slot

        pl.when(k <= 3)(lambda: ffn(k, 2))
        pl.when(k == 4)(lambda: ffn(k, 1))

        @pl.when(k >= 3)
        def _():
            for d in range(2):
                for p in range(PIECES):
                    send(slot, d, p).wait_send()

        def jc(d):
            return lax.rem(k + d * (8 - 2 * k) + 8, 8)

        def o_copy(d):
            return pltpu.make_async_copy(o_ref.at[jc(d)], big.at[ds(d, 8 * C)], osem.at[d])

        o_copy(0).start()
        o_copy(1).start()

        def combine(d, _):
            m = ma[jc(d), c, :, ds(d, TH)]
            for e in range(2 * EL):
                hit, rank = table(m, base + e)
                tm[e:e + 1, :] = rank
                tm[2 * EL + e:2 * EL + e + 1, :] = jnp.sum(jnp.where(hit, m[16:24], 0.0), axis=0, keepdims=True)
            m = tm[...].T
            io = lax.broadcasted_iota(jnp.int32, (TH, C), 1).astype(jnp.float32)
            for e in range(2 * EL):
                w = jnp.where(io == m[:, e:e + 1], m[:, 2 * EL + e:2 * EL + e + 1], 0.0)
                hi = w.astype(jnp.bfloat16)
                w = w - hi.astype(jnp.float32)
                mid = w.astype(jnp.bfloat16)
                lo = (w - mid.astype(jnp.float32)).astype(jnp.bfloat16)
                wm[0:TH, e * C:(e + 1) * C] = hi
                wm[TH:2 * TH, e * C:(e + 1) * C] = mid
                wm[2 * TH:, e * C:(e + 1) * C] = lo
            o_copy(d).wait()

            def body(nn, _):
                v = jnp.dot(wm[...], big[ds(d, 8 * C), ds(nn, B)], preferred_element_type=jnp.float32)
                part[slot, d, :, ds(nn, B)] = v[:TH] + v[TH:2 * TH] + v[2 * TH:]
                return 0

            lax.fori_loop(0, ND, body, 0)
            return 0

        lax.fori_loop(0, 2, combine, 0)

        @pl.when((k >= 3) & (k <= 7))
        def _():
            for d in range(2):
                pl.semaphore_wait(credit.at[d], 1)

        def piece(p, _):
            for d in range(2):
                @pl.when(k >= 2)
                def _():
                    send(old, d, p).wait_recv()

                    @pl.when(k <= 7)
                    def _():
                        part[slot, d, ds(p, RP), :] += recv[old, d, ds(p, RP), :]

                    @pl.when(k == 8)
                    def _():
                        v = part[slot, d, ds(p, RP), :] + recv[old, d, ds(p, RP), :]
                        y_ref[ds(d * PIECES + p, RP), :] = v.astype(y_ref.dtype)

                @pl.when(k <= 7)
                def _():
                    send(slot, d, p).start()

            return 0

        lax.fori_loop(0, PIECES, piece, 0)

        @pl.when((k >= 2) & (k <= 6))
        def _():
            for d in range(2):
                pl.semaphore_signal(credit.at[d], inc=1, device_id=prv[d], device_id_type=MESH)

        return 0

    for h in range(2):
        for d in range(2):
            gather(1, d, h, True).start()
    own(0, c).start()
    xload.wait()
    route()
    ma[0, c] = mv[...]
    for d in range(2):
        gather(1, d, 2, True).start()
    own(1, c).start()
    ffn(0, 1)
    lax.fori_loop(1, 9, step, 0)
    for d in range(2):
        for p in range(PIECES):
            send(1, d, p).wait_send()

    def drain(k, _):
        each(k, 4, lambda d, h: landed(k, d, h).wait_send())
        each(k, 4, lambda d, h: push(k, d, h, c).wait_send())
        return 0

    lax.fori_loop(1, 5, drain, 0)
    own(0, c).wait_send()
    own(1, c).wait_send()


def _experts(x, idx, wr, w1, w3, w2, C):
    EL, D, FF = w1.shape
    T = x.shape[0]
    B = min(256, FF, D)
    TH = T // 2
    bf, f32 = jnp.bfloat16, jnp.float32
    hbm = pl.BlockSpec(memory_space=pl.ANY)
    vmem = pl.BlockSpec(memory_space=pltpu.VMEM)
    dma = pltpu.SemaphoreType.DMA
    flops = 2 * 16 * EL * C * D * (3 * FF + T) + 2 * 16 * EL * C * D * 3 * T
    return pl.pallas_call(
        functools.partial(_kernel, C, B),
        out_shape=(pltpu.VMEM((T, D), bf), jax.ShapeDtypeStruct((8, 2 * EL * C, D), bf),
                   jax.ShapeDtypeStruct((8, 2, T, D), bf)),
        in_specs=[hbm, vmem, vmem, hbm, hbm, hbm],
        out_specs=(vmem, hbm, hbm),
        scratch_shapes=[
            pltpu.VMEM((2, T, D), bf),
            pltpu.VMEM((16 * C, D), bf),
            pltpu.VMEM((EL * C, T), bf),
            pltpu.VMEM((4 * C, FF), bf),
            pltpu.VMEM((2, 4 * C, D), bf),
            pltpu.VMEM((FF // B, D, B), bf),
            pltpu.VMEM((FF // B, D, B), bf),
            pltpu.VMEM((D // B, FF, B), bf),
            pltpu.VMEM((3 * TH, 2 * EL * C), bf),
            pltpu.VMEM((2, 2, TH, D), f32),
            pltpu.VMEM((2, 2, TH, D), f32),
            pltpu.VMEM((8, 2, 24, T), f32),
            pltpu.VMEM((4 * EL, TH), f32),
            pltpu.VMEM((24, T), f32),
            dma((2,)), dma((FF // B,)), dma((FF // B,)), dma((D // B,)),
            dma((EL, 2)), dma((EL, 2)), dma((5, EL, 2)), dma((2,)),
            dma((2, 2, PIECES)), dma((2, 2, PIECES)),
            dma((4, 2, 3)), dma((4, 2, 3)), dma((4, 2, 3)), dma((4, 2, 3)), dma((2,)), dma((2,)),
            pltpu.SemaphoreType.REGULAR((2,)),
        ],
        compiler_params=pltpu.CompilerParams(
            collective_id=0, has_side_effects=True, vmem_limit_bytes=58000000),
        cost_estimate=pl.CostEstimate(flops=flops, bytes_accessed=400_000_000, transcendentals=0),
    )(x, idx, wr, w1, w3, w2)[0]


def solution(mesh):
    tok = P(('data', 'outer', 'expert'), None)
    wsp = P(('outer', 'expert'), None, None)

    def local(x, wr, idx, w1, w3, w2):
        T, D = x.shape
        C = 2 * T * idx.shape[1] // wr.shape[1]
        return _experts(x, idx.T, wr.T, w1, w3, w2, C)

    return jax.shard_map(local, mesh=mesh, in_specs=(tok, P(None, None), tok, wsp, wsp, wsp), out_specs=tok, check_vma=False)
```

```python
import functools

import jax
import jax.numpy as jnp
from jax import lax
from jax.experimental import pallas as pl
from jax.experimental.pallas import tpu as pltpu
from jax.sharding import PartitionSpec as P

MESH = pl.DeviceIdType.MESH
PIECES = 4


def _kernel(C, B, x_ref, i_ref, wr_ref, w1_ref, w3_ref, w2_ref, y_ref, o_ref, xa,
            xt, big, sel, hb, ob, w1b, w3b, w2b, wm, part, recv, ma, tm, mv,
            xsem, w1sem, w3sem, w2sem, lsem, xs, xr, osem, ssem, rsem,
            ags, agr, pxs, pxr, pos, por, credit, far, ys, fsem):
    T, D = y_ref.shape
    EL, FF = w2_ref.shape[0], w2_ref.shape[1]
    TH = T // 2
    RP = TH // PIECES
    NF, ND = FF // B, D // B
    z0 = lax.axis_index('outer')
    e0 = lax.axis_index('expert')
    c = lax.rem(e0, 2)
    y0 = e0 // 2
    r = z0 + y0 * (7 - 2 * z0)

    def place(q):
        y = q // 4
        return q + y * (7 - 2 * q), y

    def dev(q):
        z, y = place(q)
        return {'outer': z, 'expert': y * 2 + c}

    nxt = (dev(lax.rem(r + 1, 8)), dev(lax.rem(r + 7, 8)))
    prv = (nxt[1], nxt[0])
    a = lax.rem(r + 1, 2)
    mid = (z0 == 1) | (z0 == 2)
    corner = jnp.logical_not(mid)
    across = dev(7 - r)
    outward = dev(lax.rem(r + 1 + 6 * (1 - a), 8))
    partner = {'outer': z0, 'expert': y0 * 2 + 1 - c}

    def ds(i, n):
        return pl.ds(pl.multiple_of(i * n, n), n)

    def w1_copy(e, cc):
        return pltpu.make_async_copy(w1_ref.at[e, :, ds(cc, B)], w1b.at[cc], w1sem.at[cc])

    def w3_copy(e, cc):
        return pltpu.make_async_copy(w3_ref.at[e, :, ds(cc, B)], w3b.at[cc], w3sem.at[cc])

    def w2_copy(e, nn):
        return pltpu.make_async_copy(w2_ref.at[e, :, ds(nn, B)], w2b.at[nn], w2sem.at[nn])

    xload = pltpu.make_async_copy(x_ref, xt.at[0], xsem.at[0])
    xload.start()
    for cc in range(NF):
        w1_copy(0, cc).start()
        w3_copy(0, cc).start()
    for nn in range(ND):
        w2_copy(0, nn).start()

    barrier = pltpu.get_barrier_semaphore()
    for d in (*nxt, partner, across):
        pl.semaphore_signal(barrier, inc=1, device_id=d, device_id_type=MESH)
    pl.semaphore_wait(barrier, 4)

    half = (ds(0, TH), ds(1, TH))
    always = ((0, 0), (1, 1), (0, 2))
    mine = (z0 * 4 + e0) * EL
    base = (z0 * 4 + y0 * 2) * EL

    def jd(k, d):
        return k + d * (8 - 2 * k)

    def block(k, d, h, core):
        if h == 2:
            return ma.at[jd(k, d), core]
        return xa.at[jd(k, d), core, half[h]]

    def gather(k, d, h, first=False):
        if first:
            src = mv if h == 2 else x_ref.at[half[h]]
        else:
            src = block(k - 1, d, h, c)
        return pltpu.make_async_remote_copy(
            src_ref=src, dst_ref=block(k, d, h, c), send_sem=ags.at[k - 1, d, h], recv_sem=agr.at[k - 1, d, h],
            device_id=nxt[d], device_id_type=MESH)

    def landed(k, d, h):
        return pltpu.make_async_remote_copy(
            src_ref=block(k, d, h, c), dst_ref=block(k, d, h, c), send_sem=ags.at[k - 1, d, h],
            recv_sem=agr.at[k - 1, d, h], device_id=nxt[d], device_id_type=MESH)

    def push(k, d, h, core):
        return pltpu.make_async_remote_copy(
            src_ref=block(k, d, h, core), dst_ref=block(k, d, h, core), send_sem=pxs.at[k - 1, d, h],
            recv_sem=pxr.at[k - 1, d, h], device_id=partner, device_id_type=MESH)

    def own(h, core):
        return pltpu.make_async_remote_copy(
            src_ref=(x_ref, mv)[h], dst_ref=(xa, ma)[h].at[0, core], send_sem=pos.at[h], recv_sem=por.at[h],
            device_id=partner, device_id_type=MESH)

    def each(k, last, f):
        for h in range(3):
            for d in range(2):
                pl.when(k <= (last if (d, h) in always else last - 1))(functools.partial(f, d, h))

    def goes(k, d):
        inner = jnp.logical_xor(corner, a == d)
        return jnp.logical_not(((k == 3) & inner) | ((k == 4) & corner & (a == d)))

    def cross(i, h):
        if i == 0:
            src, d = (mv if h == 2 else x_ref.at[half[h]]), 1 - a
        else:
            src, d = block(2, 1 - a, h, c), a
        return pltpu.make_async_remote_copy(
            src_ref=src, dst_ref=block(3, d, h, c), send_sem=ys.at[i, h], recv_sem=agr.at[2, d, h],
            device_id=across, device_id_type=MESH)

    def extra(h):
        return pltpu.make_async_remote_copy(
            src_ref=block(3, 1 - a, h, c), dst_ref=block(4, 0, h, c), send_sem=ys.at[2, h],
            recv_sem=agr.at[3, h % 2, h], device_id=outward, device_id_type=MESH)

    def each_extra(f):
        for h in range(3):
            pl.when(mid & (a == h % 2))(functools.partial(f, h))

    def arrive(k):
        def one(d, h):
            landed(k, d, h).wait_recv()
            push(k, d, h, c).start()

            @pl.when((k <= (3 if (d, h) in always else 2)) & goes(k + 1, d))
            def _():
                gather(k + 1, d, h).start()

        each(k, 4, one)

        @pl.when(mid & (k == 2))
        def _():
            for h in range(3):
                cross(1, h).start()

        @pl.when(k == 3)
        def _():
            each_extra(lambda h: extra(h).start())

    def chip(j):
        return lax.rem(r - j + 8, 8)

    def table(m, e):
        hit = m[0:8] == e.astype(jnp.float32)
        rank = jnp.sum(jnp.where(hit, m[8:16] + 1.0, 0.0), axis=0, keepdims=True) - 1.0
        return hit, rank

    def route():
        E = wr_ref.shape[0]
        ix = i_ref[...]
        logits = lax.dot_general(wr_ref[...], xt[0], (((1,), (1,)), ((), ())), preferred_element_type=jnp.float32)
        ids = lax.broadcasted_iota(jnp.int32, (E, T), 0)
        got = [jnp.sum(jnp.where(ids == ix[j:j + 1], logits, 0.0), axis=0, keepdims=True) for j in range(8)]
        top = functools.reduce(jnp.maximum, got)
        got = [jnp.exp(v - top) for v in got]
        total = functools.reduce(jnp.add, got)
        used = functools.reduce(jnp.logical_or, [ids == ix[j:j + 1] for j in range(8)])
        before = lax.broadcasted_iota(jnp.int32, (T, T), 0) < lax.broadcasted_iota(jnp.int32, (T, T), 1)
        cnt = jnp.dot(jnp.where(used, 1.0, 0.0).astype(jnp.bfloat16), jnp.where(before, 1.0, 0.0).astype(jnp.bfloat16),
                      preferred_element_type=jnp.float32)
        mv[0:8, :] = ix.astype(jnp.float32)
        for j in range(8):
            mv[8 + j:9 + j, :] = jnp.sum(jnp.where(ids == ix[j:j + 1], cnt, 0.0), axis=0, keepdims=True)
            mv[16 + j:17 + j, :] = got[j] / total

    def ffn(k, S):
        k = jnp.int32(k)
        n = 2 * S
        j0 = k
        j1 = 8 - k if S == 2 else k

        def jof(s):
            return j0 + lax.rem(s, S) * (j1 - j0)

        def core(s):
            return c + (s // S) * (1 - 2 * c)

        def x_start(s):
            pltpu.make_async_copy(xa.at[jof(s), core(s)], xt.at[lax.rem(s, 2)], xsem.at[lax.rem(s, 2)]).start()

        def x_wait(s):
            pltpu.make_async_copy(x_ref, xt.at[lax.rem(s, 2)], xsem.at[lax.rem(s, 2)]).wait()

        def dispatch(s, _):
            @pl.when(s < n - 1)
            def _():
                x_start(s + 1)

            m = ma[jof(s), core(s)]
            io = lax.broadcasted_iota(jnp.int32, (C, T), 0).astype(jnp.float32)
            for e in range(EL):
                rank = table(m, mine + e)[1]
                sel[e * C:(e + 1) * C, :] = jnp.where(rank == io, 1.0, 0.0).astype(jnp.bfloat16)

            @pl.when((k > 0) | (s > 0))
            def _():
                x_wait(s)

            def body(nn, _):
                v = jnp.dot(sel[...], xt[lax.rem(s, 2), :, ds(nn, B)], preferred_element_type=jnp.float32)
                v = v.astype(jnp.bfloat16)
                for e in range(EL):
                    big[pl.ds(pl.multiple_of(e * n * C + s * C, C), C), ds(nn, B)] = v[e * C:(e + 1) * C]
                return 0

            lax.fori_loop(0, ND, body, 0)
            return 0

        def start_first():
            x_start(jnp.int32(0))
            each(k, 4, lambda d, h: push(k, d, h, 1 - c).wait_recv())

        if S == 2:
            start_first()
        else:
            pl.when(k > 0)(start_first)

            @pl.when(k == 0)
            def _():
                own(0, 1 - c).wait_recv()
                own(1, 1 - c).wait_recv()

        lax.fori_loop(0, n, dispatch, 0)

        def local_copy(e, s):
            return pltpu.make_async_copy(
                ob.at[lax.rem(e, 2), pl.ds(s * C, C)], o_ref.at[jof(s), ds(c * EL + e, C)], lsem.at[e, s])

        def partner_copy(e, s):
            return pltpu.make_async_remote_copy(
                src_ref=ob.at[lax.rem(e, 2), pl.ds((S + s) * C, C)],
                dst_ref=o_ref.at[jof(s), ds(c * EL + e, C)],
                send_sem=xs.at[e, s], recv_sem=xr.at[k, e, s],
                device_id=partner, device_id_type=MESH)

        def arrival(e, s):
            return pltpu.make_async_remote_copy(
                src_ref=ob.at[lax.rem(e, 2), pl.ds((S + s) * C, C)],
                dst_ref=o_ref.at[jof(s), ds((1 - c) * EL + e, C)],
                send_sem=xs.at[e, s], recv_sem=xr.at[k, e, s],
                device_id=partner, device_id_type=MESH)

        def expert(e, _):
            more = k * EL + e < 5 * EL - 1
            ne = lax.rem(e + 1, EL)
            if S == 2:
                pl.when(e == EL - 1)(lambda: arrive(k + 1))

            def up(cc, _):
                w1_copy(e, cc).wait()
                w3_copy(e, cc).wait()
                xe = big[ds(e, n * C), :]
                a = jnp.dot(xe, w1b[cc], preferred_element_type=jnp.float32)
                b = jnp.dot(xe, w3b[cc], preferred_element_type=jnp.float32)
                hb[0:n * C, ds(cc, B)] = (jax.nn.silu(a) * b).astype(jnp.bfloat16)

                @pl.when(more)
                def _():
                    w1_copy(ne, cc).start()
                    w3_copy(ne, cc).start()

                return 0

            lax.fori_loop(0, NF, up, 0)

            @pl.when(e >= 2)
            def _():
                for s in range(S):
                    local_copy(e - 2, s).wait()
                    partner_copy(e - 2, s).wait_send()

            def down(nn, _):
                w2_copy(e, nn).wait()
                v = jnp.dot(hb[0:n * C, :], w2b[nn], preferred_element_type=jnp.float32)
                ob[lax.rem(e, 2), 0:n * C, ds(nn, B)] = v.astype(jnp.bfloat16)

                @pl.when(more)
                def _():
                    w2_copy(ne, nn).start()

                return 0

            lax.fori_loop(0, ND, down, 0)
            for s in range(S):
                partner_copy(e, s).start()
                local_copy(e, s).start()
            return 0

        lax.fori_loop(0, EL, expert, 0)
        if S == 1:
            pl.when(k == 0)(lambda: arrive(k + 1))
        for e in range(EL):
            for s in range(S):
                if e >= EL - 2:
                    local_copy(e, s).wait()
                    partner_copy(e, s).wait_send()
                arrival(e, s).wait_recv()

    def send(slot, d, p):
        return pltpu.make_async_remote_copy(
            src_ref=part.at[slot, d, ds(p, RP)], dst_ref=recv.at[slot, d, ds(p, RP)],
            send_sem=ssem.at[slot, d, p], recv_sem=rsem.at[slot, d, p],
            device_id=nxt[d], device_id_type=MESH)

    def hop(d, p):
        return pltpu.make_async_remote_copy(
            src_ref=part.at[1, d, ds(p, RP)], dst_ref=far.at[ds(p, RP)],
            send_sem=ssem.at[1, d, p], recv_sem=fsem.at[p],
            device_id=across, device_id_type=MESH)

    def step(k, _):
        slot = lax.rem(k, 2)
        old = 1 - slot

        pl.when(k <= 3)(lambda: ffn(k, 2))
        pl.when(k == 4)(lambda: ffn(k, 1))

        @pl.when(k >= 3)
        def _():
            for d in range(2):
                for p in range(PIECES):
                    send(slot, d, p).wait_send()

        def jc(d):
            return lax.rem(k + d * (8 - 2 * k) + 8, 8)

        def o_copy(d):
            return pltpu.make_async_copy(o_ref.at[jc(d)], big.at[ds(d, 8 * C)], osem.at[d])

        o_copy(0).start()
        o_copy(1).start()

        def combine(d, _):
            m = ma[jc(d), c, :, ds(d, TH)]
            for e in range(2 * EL):
                hit, rank = table(m, base + e)
                tm[e:e + 1, :] = rank
                tm[2 * EL + e:2 * EL + e + 1, :] = jnp.sum(jnp.where(hit, m[16:24], 0.0), axis=0, keepdims=True)
            m = tm[...].T
            io = lax.broadcasted_iota(jnp.int32, (TH, C), 1).astype(jnp.float32)
            for e in range(2 * EL):
                w = jnp.where(io == m[:, e:e + 1], m[:, 2 * EL + e:2 * EL + e + 1], 0.0)
                hi = w.astype(jnp.bfloat16)
                w = w - hi.astype(jnp.float32)
                mid = w.astype(jnp.bfloat16)
                lo = (w - mid.astype(jnp.float32)).astype(jnp.bfloat16)
                wm[0:TH, e * C:(e + 1) * C] = hi
                wm[TH:2 * TH, e * C:(e + 1) * C] = mid
                wm[2 * TH:, e * C:(e + 1) * C] = lo
            o_copy(d).wait()

            def body(nn, _):
                v = jnp.dot(wm[...], big[ds(d, 8 * C), ds(nn, B)], preferred_element_type=jnp.float32)
                part[slot, d, :, ds(nn, B)] = v[:TH] + v[TH:2 * TH] + v[2 * TH:]
                return 0

            lax.fori_loop(0, ND, body, 0)
            return 0

        lax.fori_loop(0, 2, combine, 0)

        for d in range(2):
            @pl.when((k >= 3) & (k <= 7) & jnp.logical_not(mid & (k == 3) & (a != d)))
            def _():
                pl.semaphore_wait(credit.at[d], 1)

        def piece(p, _):
            for d in range(2):
                fresh = corner & (k == 2) & (a == d)
                aside = mid & (k == 1) & (a != d)

                @pl.when((k >= 2) & jnp.logical_not(fresh))
                def _():
                    send(old, d, p).wait_recv()

                    @pl.when(k <= 7)
                    def _():
                        part[slot, d, ds(p, RP), :] += recv[old, d, ds(p, RP), :]

                    @pl.when(k == 8)
                    def _():
                        v = part[slot, d, ds(p, RP), :] + recv[old, d, ds(p, RP), :]
                        y_ref[ds(d * PIECES + p, RP), :] = v.astype(y_ref.dtype)

                @pl.when(mid & (k == 4) & (a == d))
                def _():
                    hop(d, p).wait_recv()
                    part[slot, d, ds(p, RP), :] += far[ds(p, RP), :]

                @pl.when((k <= 7) & jnp.logical_not(aside))
                def _():
                    send(slot, d, p).start()

                @pl.when(aside)
                def _():
                    hop(d, p).start()

            return 0

        lax.fori_loop(0, PIECES, piece, 0)

        for d in range(2):
            @pl.when((k >= 2) & (k <= 6) & jnp.logical_not(corner & (k == 2) & (a == d)))
            def _():
                pl.semaphore_signal(credit.at[d], inc=1, device_id=prv[d], device_id_type=MESH)

        return 0

    for h in range(2):
        for d in range(2):
            gather(1, d, h, True).start()
    own(0, c).start()

    @pl.when(mid)
    def _():
        cross(0, 0).start()
        cross(0, 1).start()

    xload.wait()
    route()
    ma[0, c] = mv[...]
    for d in range(2):
        gather(1, d, 2, True).start()
    own(1, c).start()
    pl.when(mid)(lambda: cross(0, 2).start())
    ffn(0, 1)
    lax.fori_loop(1, 9, step, 0)
    for d in range(2):
        for p in range(PIECES):
            send(1, d, p).wait_send()

    def drain(k, _):
        each(k, 4, lambda d, h: pl.when(goes(k, d))(lambda: landed(k, d, h).wait_send()))
        each(k, 4, lambda d, h: push(k, d, h, c).wait_send())
        return 0

    lax.fori_loop(1, 5, drain, 0)
    own(0, c).wait_send()
    own(1, c).wait_send()
    each_extra(lambda h: extra(h).wait_send())

    @pl.when(mid)
    def _():
        for h in range(3):
            cross(0, h).wait_send()
            cross(1, h).wait_send()


def _experts(x, idx, wr, w1, w3, w2, C):
    EL, D, FF = w1.shape
    T = x.shape[0]
    B = min(256, FF, D)
    TH = T // 2
    bf, f32 = jnp.bfloat16, jnp.float32
    hbm = pl.BlockSpec(memory_space=pl.ANY)
    vmem = pl.BlockSpec(memory_space=pltpu.VMEM)
    dma = pltpu.SemaphoreType.DMA
    flops = 2 * 16 * EL * C * D * (3 * FF + T) + 2 * 16 * EL * C * D * 3 * T
    return pl.pallas_call(
        functools.partial(_kernel, C, B),
        out_shape=(pltpu.VMEM((T, D), bf), jax.ShapeDtypeStruct((8, 2 * EL * C, D), bf),
                   jax.ShapeDtypeStruct((8, 2, T, D), bf)),
        in_specs=[hbm, vmem, vmem, hbm, hbm, hbm],
        out_specs=(vmem, hbm, hbm),
        scratch_shapes=[
            pltpu.VMEM((2, T, D), bf),
            pltpu.VMEM((16 * C, D), bf),
            pltpu.VMEM((EL * C, T), bf),
            pltpu.VMEM((4 * C, FF), bf),
            pltpu.VMEM((2, 4 * C, D), bf),
            pltpu.VMEM((FF // B, D, B), bf),
            pltpu.VMEM((FF // B, D, B), bf),
            pltpu.VMEM((D // B, FF, B), bf),
            pltpu.VMEM((3 * TH, 2 * EL * C), bf),
            pltpu.VMEM((2, 2, TH, D), f32),
            pltpu.VMEM((2, 2, TH, D), f32),
            pltpu.VMEM((8, 2, 24, T), f32),
            pltpu.VMEM((4 * EL, TH), f32),
            pltpu.VMEM((24, T), f32),
            dma((2,)), dma((FF // B,)), dma((FF // B,)), dma((D // B,)),
            dma((EL, 2)), dma((EL, 2)), dma((5, EL, 2)), dma((2,)),
            dma((2, 2, PIECES)), dma((2, 2, PIECES)),
            dma((4, 2, 3)), dma((4, 2, 3)), dma((4, 2, 3)), dma((4, 2, 3)), dma((2,)), dma((2,)),
            pltpu.SemaphoreType.REGULAR((2,)),
            pltpu.VMEM((TH, D), f32), dma((3, 3)), dma((PIECES,)),
        ],
        compiler_params=pltpu.CompilerParams(
            collective_id=0, has_side_effects=True, vmem_limit_bytes=58000000),
        cost_estimate=pl.CostEstimate(flops=flops, bytes_accessed=400_000_000, transcendentals=0),
    )(x, idx, wr, w1, w3, w2)[0]


def solution(mesh):
    tok = P(('data', 'outer', 'expert'), None)
    wsp = P(('outer', 'expert'), None, None)

    def local(x, wr, idx, w1, w3, w2):
        T, D = x.shape
        C = 2 * T * idx.shape[1] // wr.shape[1]
        return _experts(x, idx.T, wr.T, w1, w3, w2, C)

    return jax.shard_map(local, mesh=mesh, in_specs=(tok, P(None, None), tok, wsp, wsp, wsp), out_specs=tok, check_vma=False)
```

```python
import functools

import jax
import jax.numpy as jnp
from jax import lax
from jax.experimental import pallas as pl
from jax.experimental.pallas import tpu as pltpu
from jax.sharding import PartitionSpec as P

MESH = pl.DeviceIdType.MESH
PIECES = 4


def _kernel(C, B, x_ref, i_ref, wr_ref, w1_ref, w3_ref, w2_ref, y_ref, o_ref, xa,
            xt, big, sel, hb, ob, w1b, w3b, w2b, wm, part, recv, ma, tm, mv,
            xsem, w1sem, w3sem, w2sem, lsem, xs, xr, osem, ssem, rsem,
            ags, agr, pxs, pxr, pos, por, credit, far, ys, fsem):
    T, D = y_ref.shape
    EL, FF = w2_ref.shape[0], w2_ref.shape[1]
    TH = T // 2
    RP = TH // PIECES
    NF, ND = FF // B, D // B
    z0 = lax.axis_index('outer')
    e0 = lax.axis_index('expert')
    c = lax.rem(e0, 2)
    y0 = e0 // 2
    r = z0 + y0 * (7 - 2 * z0)

    def place(q):
        y = q // 4
        return q + y * (7 - 2 * q), y

    def dev(q):
        z, y = place(q)
        return {'outer': z, 'expert': y * 2 + c}

    nxt = (dev(lax.rem(r + 1, 8)), dev(lax.rem(r + 7, 8)))
    prv = (nxt[1], nxt[0])
    a = lax.rem(r + 1, 2)
    mid = (z0 == 1) | (z0 == 2)
    corner = jnp.logical_not(mid)
    across = dev(7 - r)
    outward = dev(lax.rem(r + 1 + 6 * (1 - a), 8))
    partner = {'outer': z0, 'expert': y0 * 2 + 1 - c}

    def ds(i, n):
        return pl.ds(pl.multiple_of(i * n, n), n)

    def w1_copy(e, cc):
        return pltpu.make_async_copy(w1_ref.at[e, :, ds(cc, B)], w1b.at[cc], w1sem.at[cc])

    def w3_copy(e, cc):
        return pltpu.make_async_copy(w3_ref.at[e, :, ds(cc, B)], w3b.at[cc], w3sem.at[cc])

    def w2_copy(e, nn):
        return pltpu.make_async_copy(w2_ref.at[e, :, ds(nn, B)], w2b.at[nn], w2sem.at[nn])

    xload = pltpu.make_async_copy(x_ref, xt.at[0], xsem.at[0])
    xload.start()
    for cc in range(NF):
        w1_copy(0, cc).start()
        w3_copy(0, cc).start()
    for nn in range(ND):
        w2_copy(0, nn).start()

    barrier = pltpu.get_barrier_semaphore()
    for d in (*nxt, partner, across):
        pl.semaphore_signal(barrier, inc=1, device_id=d, device_id_type=MESH)
    pl.semaphore_wait(barrier, 4)

    half = (ds(0, TH), ds(1, TH))
    always = ((0, 0), (1, 1), (0, 2))
    mine = (z0 * 4 + e0) * EL
    base = (z0 * 4 + y0 * 2) * EL

    def jd(k, d):
        return k + d * (8 - 2 * k)

    def block(k, d, h, core):
        if h == 2:
            return ma.at[jd(k, d), core]
        return xa.at[jd(k, d), core, half[h]]

    def gather(k, d, h, first=False):
        if first:
            src = mv if h == 2 else x_ref.at[half[h]]
        else:
            src = block(k - 1, d, h, c)
        return pltpu.make_async_remote_copy(
            src_ref=src, dst_ref=block(k, d, h, c), send_sem=ags.at[k - 1, d, h], recv_sem=agr.at[k - 1, d, h],
            device_id=nxt[d], device_id_type=MESH)

    def landed(k, d, h):
        return pltpu.make_async_remote_copy(
            src_ref=block(k, d, h, c), dst_ref=block(k, d, h, c), send_sem=ags.at[k - 1, d, h],
            recv_sem=agr.at[k - 1, d, h], device_id=nxt[d], device_id_type=MESH)

    def push(k, d, h, core):
        return pltpu.make_async_remote_copy(
            src_ref=block(k, d, h, core), dst_ref=block(k, d, h, core), send_sem=pxs.at[k - 1, d, h],
            recv_sem=pxr.at[k - 1, d, h], device_id=partner, device_id_type=MESH)

    def own(h, core):
        return pltpu.make_async_remote_copy(
            src_ref=(x_ref, mv)[h], dst_ref=(xa, ma)[h].at[0, core], send_sem=pos.at[h], recv_sem=por.at[h],
            device_id=partner, device_id_type=MESH)

    def each(k, last, f):
        for h in range(3):
            for d in range(2):
                pl.when(k <= (last if (d, h) in always else last - 1))(functools.partial(f, d, h))

    def goes(k, d):
        inner = jnp.logical_xor(corner, a == d)
        return jnp.logical_not(((k == 3) & inner) | ((k == 4) & corner & (a == d)))

    def cross(i, h):
        if i == 0:
            src, d = (mv if h == 2 else x_ref.at[half[h]]), 1 - a
        else:
            src, d = block(2, 1 - a, h, c), a
        return pltpu.make_async_remote_copy(
            src_ref=src, dst_ref=block(3, d, h, c), send_sem=ys.at[i, h], recv_sem=agr.at[2, d, h],
            device_id=across, device_id_type=MESH)

    def extra(h):
        return pltpu.make_async_remote_copy(
            src_ref=block(3, 1 - a, h, c), dst_ref=block(4, 0, h, c), send_sem=ys.at[2, h],
            recv_sem=agr.at[3, h % 2, h], device_id=outward, device_id_type=MESH)

    def each_extra(f):
        for h in range(3):
            pl.when(mid & (a == h % 2))(functools.partial(f, h))

    def arrive(k):
        def one(d, h):
            landed(k, d, h).wait_recv()
            push(k, d, h, c).start()

            @pl.when((k <= (3 if (d, h) in always else 2)) & goes(k + 1, d))
            def _():
                gather(k + 1, d, h).start()

        each(k, 4, one)

        @pl.when(mid & (k == 2))
        def _():
            for h in range(3):
                cross(1, h).start()

        @pl.when(k == 3)
        def _():
            each_extra(lambda h: extra(h).start())

    def chip(j):
        return lax.rem(r - j + 8, 8)

    def table(m, e):
        hit = m[0:8] == e.astype(jnp.float32)
        rank = jnp.sum(jnp.where(hit, m[8:16] + 1.0, 0.0), axis=0, keepdims=True) - 1.0
        return hit, rank

    def route():
        E = wr_ref.shape[0]
        ix = i_ref[...]
        logits = lax.dot_general(wr_ref[...], xt[0], (((1,), (1,)), ((), ())), preferred_element_type=jnp.float32)
        ids = lax.broadcasted_iota(jnp.int32, (E, T), 0)
        got = [jnp.sum(jnp.where(ids == ix[j:j + 1], logits, 0.0), axis=0, keepdims=True) for j in range(8)]
        top = functools.reduce(jnp.maximum, got)
        got = [jnp.exp(v - top) for v in got]
        total = functools.reduce(jnp.add, got)
        used = functools.reduce(jnp.logical_or, [ids == ix[j:j + 1] for j in range(8)])
        before = lax.broadcasted_iota(jnp.int32, (T, T), 0) < lax.broadcasted_iota(jnp.int32, (T, T), 1)
        cnt = jnp.dot(jnp.where(used, 1.0, 0.0).astype(jnp.bfloat16), jnp.where(before, 1.0, 0.0).astype(jnp.bfloat16),
                      preferred_element_type=jnp.float32)
        mv[0:8, :] = ix.astype(jnp.float32)
        for j in range(8):
            mv[8 + j:9 + j, :] = jnp.sum(jnp.where(ids == ix[j:j + 1], cnt, 0.0), axis=0, keepdims=True)
            mv[16 + j:17 + j, :] = got[j] / total

    def ffn(k, S):
        k = jnp.int32(k)
        n = 2 * S
        j0 = k
        j1 = 8 - k if S == 2 else k

        def jof(s):
            return j0 + lax.rem(s, S) * (j1 - j0)

        def core(s):
            return c + (s // S) * (1 - 2 * c)

        def x_start(s):
            pltpu.make_async_copy(xa.at[jof(s), core(s)], xt.at[lax.rem(s, 2)], xsem.at[lax.rem(s, 2)]).start()

        def x_wait(s):
            pltpu.make_async_copy(x_ref, xt.at[lax.rem(s, 2)], xsem.at[lax.rem(s, 2)]).wait()

        def pushed():
            each(k, 4, lambda d, h: push(k, d, h, 1 - c).wait_recv())

        def dispatch(s, _):
            @pl.when((s < n - 1) & (s != S - 1))
            def _():
                x_start(s + 1)

            m = ma[jof(s), core(s)]
            io = lax.broadcasted_iota(jnp.int32, (C, T), 0).astype(jnp.float32)
            for e in range(EL):
                rank = table(m, mine + e)[1]
                sel[e * C:(e + 1) * C, :] = jnp.where(rank == io, 1.0, 0.0).astype(jnp.bfloat16)

            @pl.when((k > 0) | (s > 0))
            def _():
                x_wait(s)

            def body(nn, _):
                v = jnp.dot(sel[...], xt[lax.rem(s, 2), :, ds(nn, B)], preferred_element_type=jnp.float32)
                v = v.astype(jnp.bfloat16)
                for e in range(EL):
                    big[pl.ds(pl.multiple_of(e * n * C + s * C, C), C), ds(nn, B)] = v[e * C:(e + 1) * C]
                return 0

            lax.fori_loop(0, ND, body, 0)

            @pl.when(s == S - 1)
            def _():
                if S == 2:
                    pushed()
                else:
                    pl.when(k > 0)(pushed)

                    @pl.when(k == 0)
                    def _():
                        own(0, 1 - c).wait_recv()
                        own(1, 1 - c).wait_recv()

                x_start(s + 1)

            return 0

        pl.when(k > 0)(lambda: x_start(jnp.int32(0)))
        lax.fori_loop(0, n, dispatch, 0)

        def local_copy(e, s):
            return pltpu.make_async_copy(
                ob.at[lax.rem(e, 2), pl.ds(s * C, C)], o_ref.at[jof(s), ds(c * EL + e, C)], lsem.at[e, s])

        def partner_copy(e, s):
            return pltpu.make_async_remote_copy(
                src_ref=ob.at[lax.rem(e, 2), pl.ds((S + s) * C, C)],
                dst_ref=o_ref.at[jof(s), ds(c * EL + e, C)],
                send_sem=xs.at[e, s], recv_sem=xr.at[k, e, s],
                device_id=partner, device_id_type=MESH)

        def arrival(e, s):
            return pltpu.make_async_remote_copy(
                src_ref=ob.at[lax.rem(e, 2), pl.ds((S + s) * C, C)],
                dst_ref=o_ref.at[jof(s), ds((1 - c) * EL + e, C)],
                send_sem=xs.at[e, s], recv_sem=xr.at[k, e, s],
                device_id=partner, device_id_type=MESH)

        def expert(e, _):
            more = k * EL + e < 5 * EL - 1
            ne = lax.rem(e + 1, EL)
            if S == 2:
                pl.when(e == EL - 1)(lambda: arrive(k + 1))

            def up(cc, _):
                w1_copy(e, cc).wait()
                w3_copy(e, cc).wait()
                xe = big[ds(e, n * C), :]
                a = jnp.dot(xe, w1b[cc], preferred_element_type=jnp.float32)
                b = jnp.dot(xe, w3b[cc], preferred_element_type=jnp.float32)
                hb[0:n * C, ds(cc, B)] = (jax.nn.silu(a) * b).astype(jnp.bfloat16)

                @pl.when(more)
                def _():
                    w1_copy(ne, cc).start()
                    w3_copy(ne, cc).start()

                return 0

            lax.fori_loop(0, NF, up, 0)

            @pl.when(e >= 2)
            def _():
                for s in range(S):
                    local_copy(e - 2, s).wait()
                    partner_copy(e - 2, s).wait_send()

            def down(nn, _):
                w2_copy(e, nn).wait()
                v = jnp.dot(hb[0:n * C, :], w2b[nn], preferred_element_type=jnp.float32)
                ob[lax.rem(e, 2), 0:n * C, ds(nn, B)] = v.astype(jnp.bfloat16)

                @pl.when(more)
                def _():
                    w2_copy(ne, nn).start()

                return 0

            lax.fori_loop(0, ND, down, 0)
            for s in range(S):
                partner_copy(e, s).start()
                local_copy(e, s).start()
            return 0

        lax.fori_loop(0, EL, expert, 0)
        if S == 1:
            pl.when(k == 0)(lambda: arrive(k + 1))
        for e in range(EL):
            for s in range(S):
                if e >= EL - 2:
                    local_copy(e, s).wait()
                    partner_copy(e, s).wait_send()
                arrival(e, s).wait_recv()

    def send(slot, d, p):
        return pltpu.make_async_remote_copy(
            src_ref=part.at[slot, d, ds(p, RP)], dst_ref=recv.at[slot, d, ds(p, RP)],
            send_sem=ssem.at[slot, d, p], recv_sem=rsem.at[slot, d, p],
            device_id=nxt[d], device_id_type=MESH)

    def hop(d, p):
        return pltpu.make_async_remote_copy(
            src_ref=part.at[1, d, ds(p, RP)], dst_ref=far.at[ds(p, RP)],
            send_sem=ssem.at[1, d, p], recv_sem=fsem.at[p],
            device_id=across, device_id_type=MESH)

    def step(k, _):
        slot = lax.rem(k, 2)
        old = 1 - slot

        pl.when(k <= 3)(lambda: ffn(k, 2))
        pl.when(k == 4)(lambda: ffn(k, 1))

        @pl.when(k >= 3)
        def _():
            for d in range(2):
                for p in range(PIECES):
                    send(slot, d, p).wait_send()

        def jc(d):
            return lax.rem(k + d * (8 - 2 * k) + 8, 8)

        def o_copy(d):
            return pltpu.make_async_copy(o_ref.at[jc(d)], big.at[ds(d, 8 * C)], osem.at[d])

        o_copy(0).start()
        o_copy(1).start()

        def combine(d, _):
            m = ma[jc(d), c, :, ds(d, TH)]
            for e in range(2 * EL):
                hit, rank = table(m, base + e)
                tm[e:e + 1, :] = rank
                tm[2 * EL + e:2 * EL + e + 1, :] = jnp.sum(jnp.where(hit, m[16:24], 0.0), axis=0, keepdims=True)
            m = tm[...].T
            io = lax.broadcasted_iota(jnp.int32, (TH, C), 1).astype(jnp.float32)
            for e in range(2 * EL):
                w = jnp.where(io == m[:, e:e + 1], m[:, 2 * EL + e:2 * EL + e + 1], 0.0)
                hi = w.astype(jnp.bfloat16)
                w = w - hi.astype(jnp.float32)
                mid = w.astype(jnp.bfloat16)
                lo = (w - mid.astype(jnp.float32)).astype(jnp.bfloat16)
                wm[0:TH, e * C:(e + 1) * C] = hi
                wm[TH:2 * TH, e * C:(e + 1) * C] = mid
                wm[2 * TH:, e * C:(e + 1) * C] = lo
            o_copy(d).wait()

            def body(nn, _):
                v = jnp.dot(wm[...], big[ds(d, 8 * C), ds(nn, B)], preferred_element_type=jnp.float32)
                part[slot, d, :, ds(nn, B)] = v[:TH] + v[TH:2 * TH] + v[2 * TH:]
                return 0

            lax.fori_loop(0, ND, body, 0)
            return 0

        lax.fori_loop(0, 2, combine, 0)

        for d in range(2):
            @pl.when((k >= 3) & (k <= 7) & jnp.logical_not(mid & (k == 3) & (a != d)))
            def _():
                pl.semaphore_wait(credit.at[d], 1)

        def piece(p, _):
            for d in range(2):
                fresh = corner & (k == 2) & (a == d)
                aside = mid & (k == 1) & (a != d)

                @pl.when((k >= 2) & jnp.logical_not(fresh))
                def _():
                    send(old, d, p).wait_recv()

                    @pl.when(k <= 7)
                    def _():
                        part[slot, d, ds(p, RP), :] += recv[old, d, ds(p, RP), :]

                    @pl.when(k == 8)
                    def _():
                        v = part[slot, d, ds(p, RP), :] + recv[old, d, ds(p, RP), :]
                        y_ref[ds(d * PIECES + p, RP), :] = v.astype(y_ref.dtype)

                @pl.when(mid & (k == 4) & (a == d))
                def _():
                    hop(d, p).wait_recv()
                    part[slot, d, ds(p, RP), :] += far[ds(p, RP), :]

                @pl.when((k <= 7) & jnp.logical_not(aside))
                def _():
                    send(slot, d, p).start()

                @pl.when(aside)
                def _():
                    hop(d, p).start()

            return 0

        lax.fori_loop(0, PIECES, piece, 0)

        for d in range(2):
            @pl.when((k >= 2) & (k <= 6) & jnp.logical_not(corner & (k == 2) & (a == d)))
            def _():
                pl.semaphore_signal(credit.at[d], inc=1, device_id=prv[d], device_id_type=MESH)

        return 0

    for h in range(2):
        for d in range(2):
            gather(1, d, h, True).start()
    own(0, c).start()

    @pl.when(mid)
    def _():
        cross(0, 0).start()
        cross(0, 1).start()

    xload.wait()
    route()
    ma[0, c] = mv[...]
    for d in range(2):
        gather(1, d, 2, True).start()
    own(1, c).start()
    pl.when(mid)(lambda: cross(0, 2).start())
    ffn(0, 1)
    lax.fori_loop(1, 9, step, 0)
    for d in range(2):
        for p in range(PIECES):
            send(1, d, p).wait_send()

    def drain(k, _):
        each(k, 4, lambda d, h: pl.when(goes(k, d))(lambda: landed(k, d, h).wait_send()))
        each(k, 4, lambda d, h: push(k, d, h, c).wait_send())
        return 0

    lax.fori_loop(1, 5, drain, 0)
    own(0, c).wait_send()
    own(1, c).wait_send()
    each_extra(lambda h: extra(h).wait_send())

    @pl.when(mid)
    def _():
        for h in range(3):
            cross(0, h).wait_send()
            cross(1, h).wait_send()


def _experts(x, idx, wr, w1, w3, w2, C):
    EL, D, FF = w1.shape
    T = x.shape[0]
    B = min(256, FF, D)
    TH = T // 2
    bf, f32 = jnp.bfloat16, jnp.float32
    hbm = pl.BlockSpec(memory_space=pl.ANY)
    vmem = pl.BlockSpec(memory_space=pltpu.VMEM)
    dma = pltpu.SemaphoreType.DMA
    flops = 2 * 16 * EL * C * D * (3 * FF + T) + 2 * 16 * EL * C * D * 3 * T
    return pl.pallas_call(
        functools.partial(_kernel, C, B),
        out_shape=(pltpu.VMEM((T, D), bf), jax.ShapeDtypeStruct((8, 2 * EL * C, D), bf),
                   jax.ShapeDtypeStruct((8, 2, T, D), bf)),
        in_specs=[hbm, vmem, vmem, hbm, hbm, hbm],
        out_specs=(vmem, hbm, hbm),
        scratch_shapes=[
            pltpu.VMEM((2, T, D), bf),
            pltpu.VMEM((16 * C, D), bf),
            pltpu.VMEM((EL * C, T), bf),
            pltpu.VMEM((4 * C, FF), bf),
            pltpu.VMEM((2, 4 * C, D), bf),
            pltpu.VMEM((FF // B, D, B), bf),
            pltpu.VMEM((FF // B, D, B), bf),
            pltpu.VMEM((D // B, FF, B), bf),
            pltpu.VMEM((3 * TH, 2 * EL * C), bf),
            pltpu.VMEM((2, 2, TH, D), f32),
            pltpu.VMEM((2, 2, TH, D), f32),
            pltpu.VMEM((8, 2, 24, T), f32),
            pltpu.VMEM((4 * EL, TH), f32),
            pltpu.VMEM((24, T), f32),
            dma((2,)), dma((FF // B,)), dma((FF // B,)), dma((D // B,)),
            dma((EL, 2)), dma((EL, 2)), dma((5, EL, 2)), dma((2,)),
            dma((2, 2, PIECES)), dma((2, 2, PIECES)),
            dma((4, 2, 3)), dma((4, 2, 3)), dma((4, 2, 3)), dma((4, 2, 3)), dma((2,)), dma((2,)),
            pltpu.SemaphoreType.REGULAR((2,)),
            pltpu.VMEM((TH, D), f32), dma((3, 3)), dma((PIECES,)),
        ],
        compiler_params=pltpu.CompilerParams(
            collective_id=0, has_side_effects=True, vmem_limit_bytes=58000000),
        cost_estimate=pl.CostEstimate(flops=flops, bytes_accessed=400_000_000, transcendentals=0),
    )(x, idx, wr, w1, w3, w2)[0]


def solution(mesh):
    tok = P(('data', 'outer', 'expert'), None)
    wsp = P(('outer', 'expert'), None, None)

    def local(x, wr, idx, w1, w3, w2):
        T, D = x.shape
        C = 2 * T * idx.shape[1] // wr.shape[1]
        return _experts(x, idx.T, wr.T, w1, w3, w2, C)

    return jax.shard_map(local, mesh=mesh, in_specs=(tok, P(None, None), tok, wsp, wsp, wsp), out_specs=tok, check_vma=False)
```
